32 devices in a mesh: gx: 16 (over z, y, core), gy: 2 (over x).
Axes of the slice: x: 2, y: 2, z: 4, core: 2. Of those that a mesh axis runs over, the one named last changes fastest.
Arguments:
- signal: float32 [45, 16, 16, 128], P(None, 'gx', 'gy'), may hold values from -6 to 6
- response: float32 [45], replicated, may hold values from 0.2 to 2
- basis: float32 [362, 45], replicated, may hold values from -0.875 to 0.875
- mask: int32 [16, 16, 128], P('gx', 'gy'), may hold values 0 or 1
- coefficients: float32 [45, 16, 16, 128], P(None, 'gx', 'gy'), may hold values from -6 to 6
- extrapolated: float32 [45, 16, 16, 128], P(None, 'gx', 'gy'), may hold values from -6 to 6
- dual_grad: float32 [3, 362, 16, 16, 128], P(None, None, 'gx', 'gy'), may hold values from -2 to 2
- dual_sign: float32 [362, 16, 16, 128], P(None, 'gx', 'gy'), may hold values from -1 to 0
Outputs:
- coefficients_out: float32 [45, 16, 16, 128], P(None, 'gx', 'gy')
- extrapolated_out: float32 [45, 16, 16, 128], P(None, 'gx', 'gy')
- dual_grad_out: float32 [3, 362, 16, 16, 128], P(None, None, 'gx', 'gy')
- dual_sign_out: float32 [362, 16, 16, 128], P(None, 'gx', 'gy')
The draws below stay inside these ranges and needn't reach their ends.
Inputs may be any that keep to these rules, and one draw needn't show every extreme that they name: `mask`: 1 marks a voxel inside the brain.
All inputs are finite; a program needn't handle non-finite values. No bound on the sum of `mask` on one device may be relied on, other than what follows from the above.
Results may differ from the reference program's by a relative error of at most 0.0001.
Values sent between devices are 32-bit elements; how exact they have to be, the bound alone decides.
No kernel may reach another device: no remote copies, remote signals or barrier semaphores. Data moves between devices by JAX's collectives and lax.ppermute only.
A program may use at most 64 MiB of HBM per device.

```python
import math
import jax
import jax.numpy as jnp
from jax import lax

NCOEF = 45
NDIR = 362
PLANES = 128
ITERS = 2
NX = 16
NY = 16


def set_ends(entries, stream_key, smallest, largest):
    index_at = [jax.random.randint(jax.random.fold_in(stream_key, axis), (), 0, length) for axis, length in enumerate(entries.shape)]
    longest = entries.shape.index(max(entries.shape))
    beside = index_at[:longest] + [(index_at[longest] + 1) % entries.shape[longest]] + index_at[longest + 1:]
    return entries.at[tuple(index_at)].set(smallest).at[tuple(beside)].set(largest)


def block_scale(rng, extent, split, least, high):
    gain = 1.0
    for axis_at, shards_of in split:
        draws = jax.random.uniform(jax.random.fold_in(jax.random.fold_in(rng, 6), axis_at), (shards_of,), jnp.float32, least / len(split), high / len(split))
        gain = gain * jnp.repeat(jnp.exp(draws), extent[axis_at] // shards_of).reshape((-1,) + (1,) * (len(extent) - 1 - axis_at))
    return gain


def noise(stream_key, shape, width, bound, pieces=(), held_as=jnp.bfloat16):
    level = block_scale(stream_key, shape, pieces, -0.22, 0.18) if pieces else 1.0
    array = jax.random.normal(stream_key, shape, jnp.float32) * width * level
    return jnp.minimum(jnp.maximum(array, -bound), bound).astype(held_as)


def setup_inputs(seed: int = 0) -> dict:
    seeds = jax.random.split(jax.random.key(seed), 9)
    signal = noise(seeds[0], (NCOEF, NX, NY, PLANES), 1.0, 6.0, ((1, 16), (2, 2)), jnp.float32)
    response = jnp.clip(jnp.exp(jax.random.uniform(seeds[1], (NCOEF,), jnp.float32, math.log(0.2), math.log(2.0))), 0.2, 2.0)
    basis = noise(seeds[2], (NDIR, NCOEF), NCOEF ** -0.5, 0.875, (), jnp.float32)
    mask = set_ends((jax.random.randint(seeds[3], (NX, NY, PLANES), 0, 4) < 3).astype(jnp.int32), jax.random.fold_in(seeds[3], 1), 0, 1)
    coefficients = noise(seeds[4], (NCOEF, NX, NY, PLANES), 1.0, 6.0, ((1, 16), (2, 2)), jnp.float32)
    extrapolated = noise(seeds[5], (NCOEF, NX, NY, PLANES), 1.0, 6.0, ((1, 16), (2, 2)), jnp.float32)
    dual_grad = noise(seeds[6], (3, NDIR, NX, NY, PLANES), 0.3, 2.0, ((2, 16), (3, 2)), jnp.float32)
    dual_sign = jnp.clip(-1.0 + 1.0 * jax.random.uniform(seeds[7], (NDIR, NX, NY, PLANES), jnp.float32) ** block_scale(seeds[7], (NDIR, NX, NY, PLANES), ((1, 16), (2, 2)), -0.2, 0.2), -1.0, 0.0)
    return {"signal": signal, "response": response, "basis": basis, "mask": mask, "coefficients": coefficients, "extrapolated": extrapolated, "dual_grad": dual_grad, "dual_sign": dual_sign}


STEP_PRIMAL = 0.25
STEP_DUAL = 0.02
TV_WEIGHT = 0.5

def to_sphere(basis, coef_rows):
    count = coef_rows.shape[0]
    result = jnp.dot(basis, coef_rows.reshape(count, -1), precision=lax.Precision.HIGHEST, preferred_element_type=jnp.float32)
    return result.reshape((basis.shape[0],) + coef_rows.shape[1:])

def to_harmonics(basis, amp_rows):
    count = amp_rows.shape[0]
    result = jnp.dot(basis.T, amp_rows.reshape(count, -1), precision=lax.Precision.HIGHEST, preferred_element_type=jnp.float32)
    return result.reshape((basis.shape[1],) + amp_rows.shape[1:])

def forward_diff(field, along):
    length = field.shape[along]
    upper_part = lax.slice_in_dim(field, 1, length, axis=along)
    lower_part = lax.slice_in_dim(field, 0, length - 1, axis=along)
    zero_face = jnp.zeros_like(lax.slice_in_dim(field, 0, 1, axis=along))
    return jnp.concatenate([upper_part - lower_part, zero_face], along)

def backward_diff(dual_part, along):
    length = dual_part.shape[along]
    kept_rows = lax.slice_in_dim(dual_part, 0, length - 1, axis=along)
    zero_face = jnp.zeros_like(lax.slice_in_dim(dual_part, 0, 1, axis=along))
    masked = jnp.concatenate([kept_rows, zero_face], along)
    before = jnp.concatenate([zero_face, kept_rows], along)
    return masked - before

def reference(signal, response, basis, mask, coefficients, extrapolated, dual_grad, dual_sign):
    weight = mask.astype(jnp.float32)[None] * response[:, None, None, None]
    target = STEP_PRIMAL * weight * signal
    divisor = 1.0 + STEP_PRIMAL * weight * response[:, None, None, None]
    for iteration in range(ITERS):
        sphere_now = to_sphere(basis, extrapolated)
        stepped = [dual_grad[spatial] + STEP_DUAL * forward_diff(sphere_now, spatial + 1) for spatial in range(3)]
        magnitude = jnp.sqrt(stepped[0] * stepped[0] + stepped[1] * stepped[1] + stepped[2] * stepped[2])
        shrink = jnp.maximum(1.0, magnitude / TV_WEIGHT)
        dual_grad = jnp.stack([part / shrink for part in stepped])
        dual_sign = jnp.minimum(0.0, dual_sign + STEP_DUAL * sphere_now)
        backward = dual_sign - (backward_diff(dual_grad[0], 1) + backward_diff(dual_grad[1], 2) + backward_diff(dual_grad[2], 3))
        trial_step = coefficients - STEP_PRIMAL * to_harmonics(basis, backward)
        updated = (trial_step + target) / divisor
        extrapolated = 2.0 * updated - coefficients
        coefficients = updated
    return (coefficients, extrapolated, dual_grad, dual_sign)
```

```python
import functools

import jax
import jax.numpy as jnp
from jax import lax
from jax.experimental import pallas as pl
from jax.experimental.pallas import tpu as pltpu
from jax.sharding import PartitionSpec as P

STEP_PRIMAL = 0.25
STEP_DUAL = 0.02
TV_WEIGHT = 0.5

F32 = jnp.float32
BF16 = jnp.bfloat16
VMEM_LIMIT = 24 * 1024 * 1024
GROUP = 16
LANES = 128


def round_up(value, unit):
    return -(-value // unit) * unit


def split_two(value):
    high = value.astype(BF16)
    low = (value - high.astype(F32)).astype(BF16)
    return high, low


def put_cat(cat_ref, value, low_row):
    rows, width = value.shape
    high, low = split_two(value)
    cat_ref[0:rows, 0:width] = high
    cat_ref[rows : 2 * rows, 0:width] = high
    cat_ref[low_row : low_row + rows, 0:width] = low


def planes_of(ref, count, rows, padded):
    parts = []
    for row in range(rows):
        part = ref[pl.ds(row, count, stride=rows), :]
        parts.append(jnp.concatenate([part, jnp.zeros((padded - count, part.shape[1]), F32)], 0))
    return jnp.concatenate(parts, 1)


def matmul(left, right):
    return jnp.dot(left, right, preferred_element_type=F32)


def wide_matmul(left_ref, right_ref, out_ref, width):
    for start in range(0, width, 256):
        size = min(256, width - start)
        out_ref[:, start : start + size] = matmul(left_ref[...], right_ref[:, start : start + size])


def harmonics(adjoint_ref, high_ref, low_ref, start, size, padded):
    first = matmul(adjoint_ref[...], high_ref[:, start : start + size])
    second = matmul(adjoint_ref[0:padded, :], low_ref[:, start : start + size])
    return first[0:padded] + first[padded : 2 * padded] + second


def all_harmonics(adjoint_ref, high_ref, low_ref, width, padded):
    parts = [
        harmonics(adjoint_ref, high_ref, low_ref, start, min(256, width - start), padded)
        for start in range(0, width, 256)
    ]
    return jnp.concatenate(parts, 1)


def last_flags():
    last_x = lax.axis_index("gx") == lax.axis_size("gx") - 1
    last_y = lax.axis_index("gy") == lax.axis_size("gy") - 1
    keep_x = jnp.where(last_x, 0.0, 1.0).astype(F32)
    keep_y = jnp.where(last_y, 0.0, 1.0).astype(F32)
    return keep_x, keep_y


def lane_edge():
    lane = lax.broadcasted_iota(jnp.int32, (GROUP, LANES), 1)
    return jnp.where(lane == LANES - 1, 0.0, 1.0).astype(F32)


def shrunk(step_x, step_y, step_z):
    square = step_x * step_x + step_y * step_y + step_z * step_z
    factor = TV_WEIGHT * lax.rsqrt(jnp.maximum(square, TV_WEIGHT * TV_WEIGHT))
    return step_x * factor, step_y * factor, step_z * factor


def next_lane(value):
    return pltpu.roll(value, LANES - 1, 1)


def previous_lane(value):
    return pltpu.roll(value, 1, 1)


class Shape:
    def __init__(self, directions, count, rows, lanes):
        assert lanes == LANES
        self.directions, self.count, self.rows = directions, count, rows
        self.padded_dirs = round_up(directions, GROUP)
        self.padded = round_up(count + 1, GROUP)
        self.width = rows * lanes
        self.low_row = round_up(2 * self.padded, LANES)
        self.depth = self.low_row + self.padded


def load_kernel(s, e_ref, basis_ref, response_ref, grad_ref, sign_ref,
                dual_ref, own_ref, cat_ref, adjoint_ref, column_ref,
                basis_in, response_in, padded_ref, e_cat, amp, sems):
    first = [
        pltpu.make_async_copy(basis_ref, basis_in, sems.at[4 * s.rows]),
        pltpu.make_async_copy(response_ref, response_in, sems.at[4 * s.rows + 1]),
        pltpu.make_async_copy(e_ref, own_ref, sems.at[4 * s.rows + 2]),
    ]
    for copy in first:
        copy.start()
    copies = []
    pad_rows = s.padded_dirs - s.directions
    for part in range(4):
        if pad_rows:
            dual_ref[part, :, s.directions :, :] = jnp.zeros((s.rows, pad_rows, LANES), F32)
    for row in range(s.rows):
        for part in (3, 1, 2, 0):
            source = sign_ref.at[:, 0, row] if part == 3 else grad_ref.at[part, :, 0, row]
            copies.append(pltpu.make_async_copy(
                source, dual_ref.at[part, row, pl.ds(0, s.directions)],
                sems.at[part * s.rows + row]))
    for copy in copies:
        copy.start()

    padded_ref[...] = jnp.zeros_like(padded_ref)
    for copy in first:
        copy.wait()
    padded_ref[0 : s.count, 0 : s.directions] = basis_in[...]
    whole = padded_ref[...]
    high, low = split_two(whole)
    adjoint_ref[0 : s.padded, :] = high[0 : s.padded, 0 : s.padded_dirs]
    adjoint_ref[s.padded : 2 * s.padded, :] = low[0 : s.padded, 0 : s.padded_dirs]
    high = high.astype(F32).T[0 : s.padded_dirs]
    low = low.astype(F32).T[0 : s.padded_dirs]
    cat_ref[:, 0:LANES] = (high + pltpu.roll(low, s.padded, 1)).astype(BF16)
    cat_ref[:, s.low_row : s.low_row + s.padded] = high[:, 0 : s.padded].astype(BF16)
    row_index = lax.broadcasted_iota(jnp.int32, (s.padded, LANES), 0)
    lane_index = lax.broadcasted_iota(jnp.int32, (s.padded, LANES), 1)
    spread = jnp.concatenate([response_in[...], jnp.zeros((1, LANES - s.count), F32)], 1)
    picked = jnp.where(row_index == lane_index, spread, 0.0)
    column_ref[...] = jnp.broadcast_to(jnp.sum(picked, 1, keepdims=True), (s.padded, LANES))

    e_cat[...] = jnp.zeros_like(e_cat)
    put_cat(e_cat, planes_of(own_ref, s.count, s.rows, s.padded) * STEP_DUAL, s.low_row)
    wide_matmul(cat_ref, e_cat, amp, s.width)
    for copy in copies:
        copy.wait()
    edge = lane_edge()

    def step(index, carry):
        here = pl.ds(pl.multiple_of(index * GROUP, GROUP), GROUP)
        values = [amp[here, row * LANES : (row + 1) * LANES] for row in range(s.rows)]
        for row in range(s.rows):
            if row + 1 < s.rows:
                dual_ref[1, row, here, :] += values[row + 1] - values[row]
            dual_ref[2, row, here, :] += (next_lane(values[row]) - values[row]) * edge
            dual_ref[3, row, here, :] = jnp.minimum(0.0, dual_ref[3, row, here, :] + values[row])
        return carry

    lax.fori_loop(0, s.padded_dirs // GROUP, step, 0)


def dual_pass(s, dual_in, dual_out, diff, amp, keep_y, highs):
    edge = lane_edge()
    back_high, back_low, x_high, x_low, y_high, y_low = highs

    def step(index, carry):
        here = pl.ds(pl.multiple_of(index * GROUP, GROUP), GROUP)
        before = None
        if amp is not None:
            value = amp[here, 0:LANES]
        for row in range(s.rows):
            at = slice(row * LANES, (row + 1) * LANES)
            step_x = dual_in[0, row, here, :] + diff[here, at]
            step_y, step_z, sign = dual_in[1, row, here, :], dual_in[2, row, here, :], dual_in[3, row, here, :]
            if row + 1 == s.rows:
                step_y = step_y + diff[here, s.width : s.width + LANES]
            if amp is not None:
                step_z = step_z + (next_lane(value) - value) * edge
                sign = jnp.minimum(0.0, sign + value)
                dual_out[3, row, here, :] = sign
                if row + 1 < s.rows:
                    after = amp[here, (row + 1) * LANES : (row + 2) * LANES]
                    step_y = step_y + (after - value)
                    value = after
            new_x, new_y, new_z = shrunk(step_x, step_y, step_z)
            dual_out[0, row, here, :] = new_x
            dual_out[1, row, here, :] = new_y
            dual_out[2, row, here, :] = new_z
            inner_z = new_z * edge
            inner_y = new_y
            if row + 1 == s.rows:
                inner_y = new_y * keep_y
                high, low = split_two(inner_y)
                y_high[here, :] = high
                y_low[here, :] = low
            back = sign - (inner_z - previous_lane(inner_z)) - inner_y
            if before is not None:
                back = back + before
            before = inner_y
            high, low = split_two(back)
            back_high[here, at] = high
            back_low[here, at] = low
            high, low = split_two(new_x)
            x_high[here, at] = high
            x_low[here, at] = low
        return carry

    lax.fori_loop(0, s.padded_dirs // GROUP, step, 0)


def weights(s, mask_ref, response_ref):
    mask = jnp.concatenate(
        [mask_ref[row : row + 1, :].astype(F32) for row in range(s.rows)], 1)
    return mask, jnp.concatenate([response_ref[...]] * s.rows, 1)


def is_odd(axis):
    return lax.rem(lax.axis_index(axis), 2) == 1


def to_partners(axis, upward, downward):
    odd = jnp.broadcast_to(is_odd(axis), upward.shape)
    return jnp.where(odd, downward, upward), jnp.where(odd, upward, downward)


def from_partners(axis, over_even, over_odd):
    odd = jnp.broadcast_to(is_odd(axis), over_even.shape)
    return jnp.where(odd, over_even, over_odd), jnp.where(odd, over_odd, over_even)


def first_kernel(s, dual_in, cat_ref, adjoint_ref, e_ref, ex_ref, ey_ref, coef_ref, signal_ref,
                 mask_ref, response_ref, dual_ref, base_ref, inverse_ref, coef_out, target_ref,
                 x_ref, v_ref, y_ref, even_ref, odd_ref,
                 e_cat, diff, back_high, back_low, x_high, x_low, y_high, y_low):
    keep_x, keep_y = last_flags()
    here = planes_of(e_ref, s.count, s.rows, s.padded)
    there = planes_of(ex_ref, s.count, s.rows, s.padded)
    edge_row = jnp.concatenate([ey_ref[...], jnp.zeros((s.padded - s.count, LANES), F32)], 0)
    e_cat[2 * s.padded : s.low_row, :] = jnp.zeros((s.low_row - 2 * s.padded, s.width + LANES), BF16)
    put_cat(e_cat, jnp.concatenate(
        [(there - here) * (STEP_DUAL * keep_x),
         (edge_row - here[:, s.width - LANES :]) * (STEP_DUAL * keep_y)], 1), s.low_row)
    wide_matmul(cat_ref, e_cat, diff, s.width + LANES)
    dual_pass(s, dual_in, dual_ref, diff, None, keep_y,
              (back_high, back_low, x_high, x_low, y_high, y_low))
    from_back = all_harmonics(adjoint_ref, back_high, back_low, s.width, s.padded)
    from_x = all_harmonics(adjoint_ref, x_high, x_low, s.width, s.padded)
    from_y = all_harmonics(adjoint_ref, y_high, y_low, LANES, s.padded)
    mask, response = weights(s, mask_ref, response_ref)
    weight = mask * response
    coef = planes_of(coef_ref, s.count, s.rows, s.padded)
    signal = planes_of(signal_ref, s.count, s.rows, s.padded)
    target = STEP_PRIMAL * weight * signal
    inverse = 1.0 / (1.0 + STEP_PRIMAL * weight * response)
    base = coef + target - STEP_PRIMAL * (from_back - keep_x * from_x)
    row_index = lax.broadcasted_iota(jnp.int32, (s.padded, s.width), 0)
    ahead = jnp.where(row_index == s.count, mask, 2.0 * base * inverse - coef)
    base_ref[...] = base
    inverse_ref[...] = inverse
    coef_out[...] = coef
    target_ref[...] = target
    x_ref[...] = from_x
    v_ref[...] = ahead
    y_ref[...] = from_y
    even_ref[...], odd_ref[...] = to_partners(
        "gy", jnp.concatenate([from_y, from_y], 0),
        jnp.concatenate([ahead[:, 0:LANES], from_x[:, 0:LANES]], 0))


def middle_kernel(s, base_in, inverse_ref, x_ref, v_ref, *refs):
    *received, base_ref, even_ref, odd_ref, side_ref = refs
    over_even = received[0][...]
    over_odd = received[1][...] if len(received) > 1 else jnp.zeros_like(over_even)
    below, above = from_partners("gy", over_even, over_odd)
    base_ref[...] = base_in[...]
    base_ref[:, 0:LANES] -= STEP_PRIMAL * below[0 : s.padded]
    side_ref[...] = above[0 : s.padded]
    ahead = v_ref[...]
    row_index = lax.broadcasted_iota(jnp.int32, (s.padded, LANES), 0)
    change = (2.0 * STEP_PRIMAL) * below[0 : s.padded] * inverse_ref[:, 0:LANES]
    change = jnp.where(row_index < s.count, change, 0.0)
    down = jnp.concatenate([ahead[:, 0:LANES] - change, ahead[:, LANES:], change], 1)
    up = jnp.concatenate([x_ref[...], above[s.padded :]], 1)
    even_ref[...], odd_ref[...] = to_partners("gx", up, down)


def ahead_of(s, message, own, response):
    row_index = lax.broadcasted_iota(jnp.int32, message.shape, 0)
    mask = message[s.count : s.count + 1, :]
    inverse = 1.0 / (1.0 + STEP_PRIMAL * (mask * response) * response)
    return jnp.where(row_index < s.count, message - (2.0 * STEP_PRIMAL) * inverse * own, 0.0)


def second_kernel(s, dual_in, cat_ref, adjoint_ref, base_ref, inverse_ref, coef_ref, target_ref,
                  x_ref, y_ref, over_even_ref, over_odd_ref, side_ref, response_ref,
                  dual_ref, base_out, coef_out, x_out, y_out,
                  e_cat, d_cat, amp, diff, back_high, back_low, x_high, x_low, y_high, y_low):
    keep_x, keep_y = last_flags()
    below, above = from_partners("gx", over_even_ref[...], over_odd_ref[...])
    response = response_ref[...]
    inverse = inverse_ref[...]
    coef = coef_ref[...]
    updated = (base_ref[...] - STEP_PRIMAL * below[:, 0 : s.width]) * inverse
    here = 2.0 * updated - coef
    wide = jnp.concatenate([response] * s.rows, 1)
    there = ahead_of(s, above[:, 0 : s.width], x_ref[...], wide)
    edge_row = ahead_of(s, side_ref[...], y_ref[...] + below[:, s.width :], response)
    zeros = jnp.zeros((s.low_row - 2 * s.padded, s.width + LANES), BF16)
    e_cat[2 * s.padded : s.low_row, :] = zeros[:, 0 : s.width]
    d_cat[2 * s.padded : s.low_row, :] = zeros
    put_cat(e_cat, here * STEP_DUAL, s.low_row)
    put_cat(d_cat, jnp.concatenate(
        [(there - here) * (STEP_DUAL * keep_x),
         (edge_row - here[:, s.width - LANES :]) * (STEP_DUAL * keep_y)], 1), s.low_row)
    wide_matmul(cat_ref, e_cat, amp, s.width)
    wide_matmul(cat_ref, d_cat, diff, s.width + LANES)
    dual_pass(s, dual_in, dual_ref, diff, amp, keep_y,
              (back_high, back_low, x_high, x_low, y_high, y_low))
    from_back = all_harmonics(adjoint_ref, back_high, back_low, s.width, s.padded)
    from_x = all_harmonics(adjoint_ref, x_high, x_low, s.width, s.padded)
    from_y = all_harmonics(adjoint_ref, y_high, y_low, LANES, s.padded)
    base_out[...] = updated + target_ref[...] - STEP_PRIMAL * (from_back - keep_x * from_x)
    coef_out[...] = updated
    x_out[...] = from_x
    y_out[...] = from_y


def store_kernel(s, dual_ref, grad_ref, sign_ref, sems):
    copies = []
    for row in range(s.rows):
        for part in range(3):
            copies.append(pltpu.make_async_copy(
                dual_ref.at[part, row, pl.ds(0, s.directions)], grad_ref.at[part, :, 0, row],
                sems.at[part * s.rows + row]))
        copies.append(pltpu.make_async_copy(
            dual_ref.at[3, row, pl.ds(0, s.directions)], sign_ref.at[:, 0, row],
            sems.at[3 * s.rows + row]))
    for copy in copies:
        copy.start()
    for copy in copies:
        copy.wait()


def last_kernel(s, base_ref, inverse_ref, coef_ref, x_ref, y_ref, coef_out, extra_out):
    total = jnp.concatenate(
        [x_ref[:, 0:LANES] + y_ref[...], x_ref[:, LANES:]], 1)
    updated = (base_ref[...] - STEP_PRIMAL * total) * inverse_ref[...]
    extra = 2.0 * updated - coef_ref[...]
    for row in range(s.rows):
        at = slice(row * LANES, (row + 1) * LANES)
        coef_out[pl.ds(row, s.count, stride=s.rows), :] = updated[0 : s.count, at]
        extra_out[pl.ds(row, s.count, stride=s.rows), :] = extra[0 : s.count, at]


def call(kernel, outs, ins, scratch, name, flops, in_specs=None, out_specs=None, aliases=None):
    vmem = pl.BlockSpec(memory_space=pltpu.VMEM)
    count = len(outs) if isinstance(outs, (tuple, list)) else 1
    size = lambda arrays: sum(a.size * a.dtype.itemsize for a in jax.tree.leaves(arrays))
    return pl.pallas_call(
        kernel,
        out_shape=outs,
        in_specs=in_specs or [vmem] * len(ins),
        out_specs=out_specs or ([vmem] * count if isinstance(outs, (tuple, list)) else vmem),
        scratch_shapes=scratch,
        input_output_aliases=aliases or {},
        compiler_params=pltpu.CompilerParams(vmem_limit_bytes=VMEM_LIMIT),
        cost_estimate=pl.CostEstimate(
            flops=flops, bytes_accessed=size(outs) + size(list(ins)), transcendentals=0),
        name=name,
    )(*ins)


def pair_lists(count):
    even = [pair for low in range(0, count - 1, 2) for pair in ((low, low + 1), (low + 1, low))]
    odd = [pair for low in range(1, count - 1, 2) for pair in ((low, low + 1), (low + 1, low))]
    return even, odd


def exchange(axis, to_even, to_odd):
    even, odd = pair_lists(lax.axis_size(axis))
    received = [lax.ppermute(to_odd, axis, odd)] if odd else []
    return [lax.ppermute(to_even, axis, even)] + received


def shift(value, axis, steps):
    count = lax.axis_size(axis)
    pairs = [(i, i + steps) for i in range(count) if 0 <= i + steps < count]
    return lax.ppermute(value, axis, pairs)


def per_device(signal, response, basis, mask, coefficients, extrapolated, dual_grad, dual_sign):
    count, layers, rows, lanes = signal.shape
    assert layers == 1
    s = Shape(basis.shape[0], count, rows, lanes)
    flat = lambda a: a.reshape(count * rows, lanes)
    f32 = lambda *shape: jax.ShapeDtypeStruct(shape, F32)
    bf16 = lambda *shape: jax.ShapeDtypeStruct(shape, BF16)
    vmem = pl.BlockSpec(memory_space=pltpu.VMEM)
    hbm = pl.BlockSpec(memory_space=pltpu.HBM)
    dirs, padded, width = s.padded_dirs, s.padded, s.width
    splits = [pltpu.VMEM((dirs, width), BF16)] * 4 + [pltpu.VMEM((dirs, LANES), BF16)] * 2
    dual = f32(4, rows, dirs, lanes)
    plane = f32(padded, width)

    after_x = shift(extrapolated, "gx", -1)
    after_y = shift(extrapolated[:, 0, 0], "gy", -1)
    in_hbm = lambda a: pltpu.with_memory_space_constraint(a, pltpu.HBM)
    line = f32(padded, lanes)
    duals, own, cat, adjoint, column = call(
        functools.partial(load_kernel, s),
        (dual, f32(count * rows, lanes), bf16(dirs, s.depth), bf16(2 * padded, dirs), line),
        [in_hbm(a) for a in
         (flat(extrapolated), basis.T, response[None], dual_grad, dual_sign)],
        [pltpu.VMEM((count, s.directions), F32), pltpu.VMEM((1, count), F32),
         pltpu.VMEM((LANES, round_up(dirs, LANES)), F32), pltpu.VMEM((s.depth, width), BF16),
         pltpu.VMEM((dirs, width), F32), pltpu.SemaphoreType.DMA((4 * rows + 3,))],
        "load", 2_000_000_000, in_specs=[hbm] * 5)
    duals, base, inverse, coef, target, from_x, ahead, from_y, to_even, to_odd = call(
        functools.partial(first_kernel, s),
        (dual,) + (plane,) * 6 + (line, f32(2 * padded, lanes), f32(2 * padded, lanes)),
        (duals, cat, adjoint, own, flat(after_x), after_y, flat(coefficients), flat(signal),
         mask[0], column),
        [pltpu.VMEM((s.depth, width + LANES), BF16), pltpu.VMEM((dirs, width + LANES), F32)] + splits,
        "first", 2_000_000_000, aliases={0: 0})
    message = f32(padded, width + lanes)
    base, to_even, to_odd, side = call(
        functools.partial(middle_kernel, s),
        (plane, message, message, line),
        [base, inverse, from_x, ahead] + exchange("gy", to_even, to_odd), [], "middle", 1_000_000)
    over_even, over_odd = exchange("gx", to_even, to_odd)
    duals, base, coef, from_x, from_y = call(
        functools.partial(second_kernel, s),
        (dual, plane, plane, plane, line),
        (duals, cat, adjoint, base, inverse, coef, target, from_x, from_y, over_even, over_odd,
         side, column),
        [pltpu.VMEM((s.depth, width), BF16), pltpu.VMEM((s.depth, width + LANES), BF16),
         pltpu.VMEM((dirs, width), F32), pltpu.VMEM((dirs, width + LANES), F32)] + splits,
        "second", 2_000_000_000, aliases={0: 0})
    below_x = shift(from_x, "gx", 1)
    below_y = shift(from_y, "gy", 1)
    grad_out, sign_out = call(
        functools.partial(store_kernel, s),
        (f32(*dual_grad.shape), f32(*dual_sign.shape)), (duals,),
        [pltpu.SemaphoreType.DMA((4 * rows,))], "store", 2_000_000_000, out_specs=[hbm, hbm])
    coef_out, extra_out = call(
        functools.partial(last_kernel, s),
        (f32(count * rows, lanes), f32(count * rows, lanes)),
        (base, inverse, coef, below_x, below_y), [], "last", 1_000_000)
    return (coef_out.reshape(signal.shape), extra_out.reshape(signal.shape), grad_out, sign_out)


def solution(mesh):
    cube = P(None, "gx", "gy", None)
    in_specs = (cube, P(), P(), P("gx", "gy", None), cube, cube, P(None, None, "gx", "gy", None), cube)
    out_specs = (cube, cube, P(None, None, "gx", "gy", None), cube)
    return jax.shard_map(per_device, mesh=mesh, in_specs=in_specs, out_specs=out_specs, check_vma=False)
```

```python
import functools

import jax
import jax.numpy as jnp
from jax import lax
from jax.experimental import pallas as pl
from jax.experimental.pallas import tpu as pltpu
from jax.sharding import PartitionSpec as P

STEP_PRIMAL = 0.25
STEP_DUAL = 0.02
TV_WEIGHT = 0.5

F32 = jnp.float32
BF16 = jnp.bfloat16
VMEM_LIMIT = 24 * 1024 * 1024
GROUP = 16
LANES = 128


def round_up(value, unit):
    return -(-value // unit) * unit


def split_two(value):
    high = value.astype(BF16)
    low = (value - high.astype(F32)).astype(BF16)
    return high, low


def put_cat(cat_ref, value, low_row):
    rows, width = value.shape
    high, low = split_two(value)
    cat_ref[0:rows, 0:width] = high
    cat_ref[rows : 2 * rows, 0:width] = high
    cat_ref[low_row : low_row + rows, 0:width] = low


def planes_of(ref, count, rows, padded):
    parts = []
    for row in range(rows):
        part = ref[pl.ds(row, count, stride=rows), :]
        parts.append(jnp.concatenate([part, jnp.zeros((padded - count, part.shape[1]), F32)], 0))
    return jnp.concatenate(parts, 1)


def matmul(left, right):
    return jnp.dot(left, right, preferred_element_type=F32)


def wide_matmul(left_ref, right_ref, out_ref, width):
    for start in range(0, width, 256):
        size = min(256, width - start)
        out_ref[:, start : start + size] = matmul(left_ref[...], right_ref[:, start : start + size])


def harmonics(adjoint_ref, high_ref, low_ref, start, size, padded):
    first = matmul(adjoint_ref[...], high_ref[:, start : start + size])
    second = matmul(adjoint_ref[0:padded, :], low_ref[:, start : start + size])
    return first[0:padded] + first[padded : 2 * padded] + second


def all_harmonics(adjoint_ref, high_ref, low_ref, width, padded):
    parts = [
        harmonics(adjoint_ref, high_ref, low_ref, start, min(256, width - start), padded)
        for start in range(0, width, 256)
    ]
    return jnp.concatenate(parts, 1)


def last_flags():
    last_x = lax.axis_index("gx") == lax.axis_size("gx") - 1
    last_y = lax.axis_index("gy") == lax.axis_size("gy") - 1
    keep_x = jnp.where(last_x, 0.0, 1.0).astype(F32)
    keep_y = jnp.where(last_y, 0.0, 1.0).astype(F32)
    return keep_x, keep_y


def lane_edge():
    lane = lax.broadcasted_iota(jnp.int32, (GROUP, LANES), 1)
    return jnp.where(lane == LANES - 1, 0.0, 1.0).astype(F32)


def shrunk(step_x, step_y, step_z):
    square = step_x * step_x + step_y * step_y + step_z * step_z
    factor = TV_WEIGHT * lax.rsqrt(jnp.maximum(square, TV_WEIGHT * TV_WEIGHT))
    return step_x * factor, step_y * factor, step_z * factor


def next_lane(value):
    return pltpu.roll(value, LANES - 1, 1)


def previous_lane(value):
    return pltpu.roll(value, 1, 1)


class Shape:
    def __init__(self, directions, count, rows, lanes):
        assert lanes == LANES
        self.directions, self.count, self.rows = directions, count, rows
        self.padded_dirs = round_up(directions, GROUP)
        self.padded = round_up(count + 1, GROUP)
        self.width = rows * lanes
        self.low_row = round_up(2 * self.padded, LANES)
        self.depth = self.low_row + self.padded
        self.groups = self.padded_dirs // GROUP
        self.part_rows = (rows + 1) * self.padded_dirs + 8

    def start(self, part, row):
        return part * self.part_rows + (row + 1) * self.padded_dirs

    def at(self, part, row, index):
        return pl.ds(pl.multiple_of(self.start(part, row) + index * GROUP, 8), GROUP)

    def lanes(self, row):
        return pl.ds(pl.multiple_of(row * LANES, LANES), LANES)


def load_kernel(s, e_ref, basis_ref, response_ref, grad_ref, sign_ref,
                dual_ref, sign_out, own_ref, cat_ref, adjoint_ref, column_ref,
                basis_in, response_in, padded_ref, e_cat, amp, sems):
    first = [
        pltpu.make_async_copy(basis_ref, basis_in, sems.at[4 * s.rows]),
        pltpu.make_async_copy(response_ref, response_in, sems.at[4 * s.rows + 1]),
        pltpu.make_async_copy(e_ref, own_ref, sems.at[4 * s.rows + 2]),
    ]
    for copy in first:
        copy.start()
    pad_rows = s.padded_dirs - s.directions
    for part in range(4):
        for row in range(s.rows):
            if pad_rows:
                end = s.start(part % 3, row) + s.padded_dirs
                place = sign_out if part == 3 else dual_ref
                place[end - pad_rows : end, :] = jnp.zeros((pad_rows, LANES), F32)

    def copy_of(part, row):
        source = sign_ref.at[:, 0, row] if part == 3 else grad_ref.at[part, :, 0, row]
        place = sign_out if part == 3 else dual_ref
        target = place.at[pl.ds(s.start(part % 3, row), s.directions)]
        return pltpu.make_async_copy(source, target, sems.at[part * s.rows + row])

    for row in range(s.rows):
        for part in (1, 2, 3):
            copy_of(part, row).start()
    for row in range(s.rows):
        copy_of(0, row).start()

    padded_ref[...] = jnp.zeros_like(padded_ref)
    for copy in first:
        copy.wait()
    padded_ref[0 : s.count, 0 : s.directions] = basis_in[...]
    whole = padded_ref[...]
    high, low = split_two(whole)
    adjoint_ref[0 : s.padded, :] = high[0 : s.padded, 0 : s.padded_dirs]
    adjoint_ref[s.padded : 2 * s.padded, :] = low[0 : s.padded, 0 : s.padded_dirs]
    high = high.astype(F32).T[0 : s.padded_dirs]
    low = low.astype(F32).T[0 : s.padded_dirs]
    cat_ref[:, 0:LANES] = (high + pltpu.roll(low, s.padded, 1)).astype(BF16)
    cat_ref[:, s.low_row : s.low_row + s.padded] = high[:, 0 : s.padded].astype(BF16)
    row_index = lax.broadcasted_iota(jnp.int32, (s.padded, LANES), 0)
    lane_index = lax.broadcasted_iota(jnp.int32, (s.padded, LANES), 1)
    spread = jnp.concatenate([response_in[...], jnp.zeros((1, LANES - s.count), F32)], 1)
    picked = jnp.where(row_index == lane_index, spread, 0.0)
    column_ref[...] = jnp.broadcast_to(jnp.sum(picked, 1, keepdims=True), (s.padded, LANES))

    e_cat[...] = jnp.zeros_like(e_cat)
    put_cat(e_cat, planes_of(own_ref, s.count, s.rows, s.padded) * STEP_DUAL, s.low_row)
    wide_matmul(cat_ref, e_cat, amp, s.width)
    edge = lane_edge()

    def update_row(row):
        for part in (1, 2, 3):
            copy_of(part, row).wait()
        for index in range(s.groups):
            here = slice(index * GROUP, (index + 1) * GROUP)
            value = amp[here, s.lanes(row)]
            if not isinstance(row, int):
                dual_ref[s.at(1, row, index), :] += amp[here, s.lanes(row + 1)] - value
            dual_ref[s.at(2, row, index), :] += (next_lane(value) - value) * edge
            sign = sign_out[s.at(0, row, index), :] + value
            sign_out[s.at(0, row, index), :] = jnp.minimum(0.0, sign)

    def step(row, carry):
        update_row(row)
        return carry

    lax.fori_loop(0, s.rows - 1, step, 0)
    update_row(s.rows - 1)
    for row in range(s.rows):
        copy_of(0, row).wait()


def dual_pass(s, dual_in, sign_in, dual_out, sign_out, change, highs):
    edge = lane_edge()
    back_high, back_low, x_high, x_low, y_high, y_low = highs
    full = sign_out is not None
    signs = sign_out if full else sign_in
    dual_out[s.start(1, -1) : s.start(1, 0), :] = jnp.zeros((s.padded_dirs, LANES), F32)

    def part_lanes(part, row):
        return pl.ds(pl.multiple_of(part * s.width + row * LANES, LANES), LANES)

    def shrink_row(row):
        for index in range(s.groups):
            here = slice(index * GROUP, (index + 1) * GROUP)
            step_x = dual_in[s.at(0, row, index), :] + change[here, part_lanes(0, row)]
            step_y, step_z = dual_in[s.at(1, row, index), :], dual_in[s.at(2, row, index), :]
            if full:
                step_y = step_y + change[here, part_lanes(1, row)]
                step_z = step_z + change[here, part_lanes(2, row)]
                sign_out[s.at(0, row, index), :] = jnp.minimum(
                    0.0, sign_in[s.at(0, row, index), :] + change[here, part_lanes(3, row)])
            elif isinstance(row, int):
                step_y = step_y + change[here, part_lanes(1, 0)]
            new_x, new_y, new_z = shrunk(step_x, step_y, step_z)
            dual_out[s.at(0, row, index), :] = new_x
            dual_out[s.at(1, row, index), :] = new_y
            dual_out[s.at(2, row, index), :] = new_z

    def split_row(row, carry):
        for index in range(s.groups):
            here = slice(index * GROUP, (index + 1) * GROUP)
            inner_z = dual_out[s.at(2, row, index), :] * edge
            back = signs[s.at(0, row, index), :] - (inner_z - previous_lane(inner_z))
            back = back - (dual_out[s.at(1, row, index), :] - dual_out[s.at(1, row - 1, index), :])
            back_high[here, s.lanes(row)], back_low[here, s.lanes(row)] = split_two(back)
            x_high[here, s.lanes(row)], x_low[here, s.lanes(row)] = split_two(
                dual_out[s.at(0, row, index), :])
        return carry

    def step(row, carry):
        shrink_row(row)
        return carry

    if full:
        lax.fori_loop(0, s.rows, step, 0)
    else:
        lax.fori_loop(0, s.rows - 1, step, 0)
        shrink_row(s.rows - 1)
    lax.fori_loop(0, s.rows, split_row, 0)
    for index in range(s.groups):
        here = slice(index * GROUP, (index + 1) * GROUP)
        y_high[here, :], y_low[here, :] = split_two(dual_out[s.at(1, s.rows - 1, index), :])


def all_adjoints(s, adjoint_ref, splits, keep_x, keep_y):
    back_high, back_low, x_high, x_low, y_high, y_low = splits
    from_back = all_harmonics(adjoint_ref, back_high, back_low, s.width, s.padded)
    from_x = all_harmonics(adjoint_ref, x_high, x_low, s.width, s.padded)
    from_y = all_harmonics(adjoint_ref, y_high, y_low, LANES, s.padded)
    last = from_back[:, s.width - LANES :] + (1.0 - keep_y) * from_y
    total = jnp.concatenate([from_back[:, : s.width - LANES], last], 1) - keep_x * from_x
    return total, from_x, from_y


def weights(s, mask_ref, response_ref):
    mask = jnp.concatenate(
        [mask_ref[row : row + 1, :].astype(F32) for row in range(s.rows)], 1)
    return mask, jnp.concatenate([response_ref[...]] * s.rows, 1)


def is_odd(axis):
    return lax.rem(lax.axis_index(axis), 2) == 1


def to_partners(axis, upward, downward):
    odd = jnp.broadcast_to(is_odd(axis), upward.shape)
    return jnp.where(odd, downward, upward), jnp.where(odd, upward, downward)


def from_partners(axis, over_even, over_odd):
    odd = jnp.broadcast_to(is_odd(axis), over_even.shape)
    return jnp.where(odd, over_even, over_odd), jnp.where(odd, over_odd, over_even)


def first_kernel(s, dual_in, sign_in, cat_ref, adjoint_ref, e_ref, ex_ref, ey_ref, coef_ref, signal_ref,
                 mask_ref, response_ref, dual_ref, base_ref, inverse_ref, coef_out, target_ref,
                 x_ref, v_ref, y_ref, *refs):
    e_cat, diff = refs[-8:-6]
    send_refs = refs[:-8]
    keep_x, keep_y = last_flags()
    here = planes_of(e_ref, s.count, s.rows, s.padded)
    there = planes_of(ex_ref, s.count, s.rows, s.padded)
    edge_row = jnp.concatenate([ey_ref[...], jnp.zeros((s.padded - s.count, LANES), F32)], 0)
    e_cat[2 * s.padded : s.low_row, :] = jnp.zeros((s.low_row - 2 * s.padded, s.width + LANES), BF16)
    put_cat(e_cat, jnp.concatenate(
        [(there - here) * (STEP_DUAL * keep_x),
         (edge_row - here[:, s.width - LANES :]) * (STEP_DUAL * keep_y)], 1), s.low_row)
    wide_matmul(cat_ref, e_cat, diff, s.width + LANES)
    dual_pass(s, dual_in, sign_in, dual_ref, None, diff, refs[-6:])
    total, from_x, from_y = all_adjoints(s, adjoint_ref, refs[-6:], keep_x, keep_y)
    mask, response = weights(s, mask_ref, response_ref)
    weight = mask * response
    coef = planes_of(coef_ref, s.count, s.rows, s.padded)
    signal = planes_of(signal_ref, s.count, s.rows, s.padded)
    target = STEP_PRIMAL * weight * signal
    inverse = 1.0 / (1.0 + STEP_PRIMAL * weight * response)
    base = coef + target - STEP_PRIMAL * total
    row_index = lax.broadcasted_iota(jnp.int32, (s.padded, s.width), 0)
    ahead = jnp.where(row_index == s.count, mask, 2.0 * base * inverse - coef)
    base_ref[...] = base
    inverse_ref[...] = inverse
    coef_out[...] = coef
    target_ref[...] = target
    x_ref[...] = from_x
    v_ref[...] = ahead
    y_ref[...] = from_y
    sends = to_partners(
        "gy", jnp.concatenate([from_y, from_y], 0),
        jnp.concatenate([ahead[:, 0:LANES], from_x[:, 0:LANES]], 0))
    for send_ref, send in zip(send_refs, sends):
        send_ref[...] = send


def middle_kernel(s, base_in, inverse_ref, x_ref, v_ref, *refs):
    *received, base_ref, even_ref, odd_ref, side_ref = refs
    over_even = received[0][...]
    over_odd = received[1][...] if len(received) > 1 else jnp.zeros_like(over_even)
    below, above = from_partners("gy", over_even, over_odd)
    base_ref[...] = base_in[...]
    base_ref[:, 0:LANES] -= STEP_PRIMAL * below[0 : s.padded]
    side_ref[...] = above[0 : s.padded]
    ahead = v_ref[...]
    row_index = lax.broadcasted_iota(jnp.int32, (s.padded, LANES), 0)
    change = (2.0 * STEP_PRIMAL) * below[0 : s.padded] * inverse_ref[:, 0:LANES]
    change = jnp.where(row_index < s.count, change, 0.0)
    down = jnp.concatenate([ahead[:, 0:LANES] - change, ahead[:, LANES:], change], 1)
    up = jnp.concatenate([x_ref[...], above[s.padded :]], 1)
    even_ref[...], odd_ref[...] = to_partners("gx", up, down)


def ahead_of(s, message, own, response):
    row_index = lax.broadcasted_iota(jnp.int32, message.shape, 0)
    mask = message[s.count : s.count + 1, :]
    inverse = 1.0 / (1.0 + STEP_PRIMAL * (mask * response) * response)
    return jnp.where(row_index < s.count, message - (2.0 * STEP_PRIMAL) * inverse * own, 0.0)


def second_kernel(s, dual_in, sign_in, cat_ref, adjoint_ref, base_ref, inverse_ref, coef_ref, target_ref,
                  x_ref, y_ref, over_even_ref, over_odd_ref, side_ref, response_ref,
                  dual_ref, sign_ref, base_out, coef_out, x_out, y_out,
                  e_cat, change, *splits):
    keep_x, keep_y = last_flags()
    below, above = from_partners("gx", over_even_ref[...], over_odd_ref[...])
    response = response_ref[...]
    inverse = inverse_ref[...]
    coef = coef_ref[...]
    updated = (base_ref[...] - STEP_PRIMAL * below[:, 0 : s.width]) * inverse
    here = 2.0 * updated - coef
    wide = jnp.concatenate([response] * s.rows, 1)
    there = ahead_of(s, above[:, 0 : s.width], x_ref[...], wide)
    edge_row = ahead_of(s, side_ref[...], y_ref[...] + below[:, s.width :], response)
    e_cat[2 * s.padded : s.low_row, :] = jnp.zeros((s.low_row - 2 * s.padded, 4 * s.width), BF16)
    edge = lane_edge()[0:1]
    planes = [here[:, row * LANES : (row + 1) * LANES] for row in range(s.rows)]
    along_y = jnp.concatenate([here[:, LANES:], edge_row], 1) - here
    along_y = jnp.concatenate(
        [along_y[:, : s.width - LANES], keep_y * along_y[:, s.width - LANES :]], 1)
    along_z = jnp.concatenate([(next_lane(plane) - plane) * edge for plane in planes], 1)
    put_cat(e_cat, STEP_DUAL * jnp.concatenate(
        [(there - here) * keep_x, along_y, along_z, here], 1), s.low_row)
    wide_matmul(cat_ref, e_cat, change, 4 * s.width)
    dual_pass(s, dual_in, sign_in, dual_ref, sign_ref, change, splits)
    total, from_x, from_y = all_adjoints(s, adjoint_ref, splits, keep_x, keep_y)
    base_out[...] = updated + target_ref[...] - STEP_PRIMAL * total
    coef_out[...] = updated
    x_out[...] = from_x
    y_out[...] = from_y


def store_kernel(s, dual_ref, sign_in, grad_ref, sign_ref, sems):
    copies = []
    for row in range(s.rows):
        for part in range(3):
            copies.append(pltpu.make_async_copy(
                dual_ref.at[pl.ds(s.start(part, row), s.directions)], grad_ref.at[part, :, 0, row],
                sems.at[part * s.rows + row]))
        copies.append(pltpu.make_async_copy(
            sign_in.at[pl.ds(s.start(0, row), s.directions)], sign_ref.at[:, 0, row],
            sems.at[3 * s.rows + row]))
    for copy in copies:
        copy.start()
    for copy in copies:
        copy.wait()


def last_kernel(s, base_ref, inverse_ref, coef_ref, x_ref, y_ref, coef_out, extra_out):
    total = jnp.concatenate(
        [x_ref[:, 0:LANES] + y_ref[...], x_ref[:, LANES:]], 1)
    updated = (base_ref[...] - STEP_PRIMAL * total) * inverse_ref[...]
    extra = 2.0 * updated - coef_ref[...]
    for row in range(s.rows):
        at = slice(row * LANES, (row + 1) * LANES)
        coef_out[pl.ds(row, s.count, stride=s.rows), :] = updated[0 : s.count, at]
        extra_out[pl.ds(row, s.count, stride=s.rows), :] = extra[0 : s.count, at]


def call(kernel, outs, ins, scratch, name, flops, in_specs=None, out_specs=None, aliases=None):
    vmem = pl.BlockSpec(memory_space=pltpu.VMEM)
    count = len(outs) if isinstance(outs, (tuple, list)) else 1
    size = lambda arrays: sum(a.size * a.dtype.itemsize for a in jax.tree.leaves(arrays))
    return pl.pallas_call(
        kernel,
        out_shape=outs,
        in_specs=in_specs or [vmem] * len(ins),
        out_specs=out_specs or ([vmem] * count if isinstance(outs, (tuple, list)) else vmem),
        scratch_shapes=scratch,
        input_output_aliases=aliases or {},
        compiler_params=pltpu.CompilerParams(vmem_limit_bytes=VMEM_LIMIT),
        cost_estimate=pl.CostEstimate(
            flops=flops, bytes_accessed=size(outs) + size(list(ins)), transcendentals=0),
        name=name,
    )(*ins)


def pair_lists(count):
    even = [pair for low in range(0, count - 1, 2) for pair in ((low, low + 1), (low + 1, low))]
    odd = [pair for low in range(1, count - 1, 2) for pair in ((low, low + 1), (low + 1, low))]
    return [even, odd] if odd else [even]


def exchange(axis, sends):
    lists = pair_lists(lax.axis_size(axis))
    return [lax.ppermute(send, axis, pairs) for send, pairs in zip(sends, lists)]


def shift(value, axis, steps):
    count = lax.axis_size(axis)
    pairs = [(i, i + steps) for i in range(count) if 0 <= i + steps < count]
    return lax.ppermute(value, axis, pairs)


def per_device(signal, response, basis, mask, coefficients, extrapolated, dual_grad, dual_sign):
    count, layers, rows, lanes = signal.shape
    assert layers == 1
    s = Shape(basis.shape[0], count, rows, lanes)
    flat = lambda a: a.reshape(count * rows, lanes)
    f32 = lambda *shape: jax.ShapeDtypeStruct(shape, F32)
    bf16 = lambda *shape: jax.ShapeDtypeStruct(shape, BF16)
    vmem = pl.BlockSpec(memory_space=pltpu.VMEM)
    hbm = pl.BlockSpec(memory_space=pltpu.HBM)
    dirs, padded, width = s.padded_dirs, s.padded, s.width
    splits = [pltpu.VMEM((dirs, width), BF16)] * 4 + [pltpu.VMEM((dirs, LANES), BF16)] * 2
    dual = f32(3 * s.part_rows, lanes)
    signs = f32(s.part_rows, lanes)
    plane = f32(padded, width)

    after_x = shift(extrapolated, "gx", -1)
    after_y = shift(extrapolated[:, 0, 0], "gy", -1)
    in_hbm = lambda a: pltpu.with_memory_space_constraint(a, pltpu.HBM)
    line = f32(padded, lanes)
    duals, sign, own, cat, adjoint, column = call(
        functools.partial(load_kernel, s),
        (dual, signs, f32(count * rows, lanes), bf16(dirs, s.depth), bf16(2 * padded, dirs), line),
        [in_hbm(a) for a in
         (flat(extrapolated), basis.T, response[None], dual_grad, dual_sign)],
        [pltpu.VMEM((count, s.directions), F32), pltpu.VMEM((1, count), F32),
         pltpu.VMEM((LANES, round_up(dirs, LANES)), F32), pltpu.VMEM((s.depth, width), BF16),
         pltpu.VMEM((dirs, width), F32), pltpu.SemaphoreType.DMA((4 * rows + 3,))],
        "load", 2_000_000_000, in_specs=[hbm] * 5)
    pairs_y = len(pair_lists(lax.axis_size("gy")))
    duals, base, inverse, coef, target, from_x, ahead, from_y, *sends = call(
        functools.partial(first_kernel, s),
        (dual,) + (plane,) * 6 + (line,) + (f32(2 * padded, lanes),) * pairs_y,
        (duals, sign, cat, adjoint, own, flat(after_x), after_y, flat(coefficients), flat(signal),
         mask[0], column),
        [pltpu.VMEM((s.depth, width + LANES), BF16), pltpu.VMEM((dirs, width + LANES), F32)] + splits,
        "first", 2_000_000_000)
    message = f32(padded, width + lanes)
    base, to_even, to_odd, side = call(
        functools.partial(middle_kernel, s),
        (plane, message, message, line),
        [base, inverse, from_x, ahead] + exchange("gy", sends), [], "middle", 1_000_000)
    over_even, over_odd = exchange("gx", [to_even, to_odd])
    duals, sign, base, coef, from_x, from_y = call(
        functools.partial(second_kernel, s),
        (dual, signs, plane, plane, plane, line),
        (duals, sign, cat, adjoint, base, inverse, coef, target, from_x, from_y, over_even, over_odd,
         side, column),
        [pltpu.VMEM((s.depth, 4 * width), BF16), pltpu.VMEM((dirs, 4 * width), F32)] + splits,
        "second", 2_000_000_000)
    below_x = shift(from_x, "gx", 1)
    below_y = shift(from_y, "gy", 1)
    grad_out, sign_out = call(
        functools.partial(store_kernel, s),
        (f32(*dual_grad.shape), f32(*dual_sign.shape)), (duals, sign),
        [pltpu.SemaphoreType.DMA((4 * rows,))], "store", 2_000_000_000, out_specs=[hbm, hbm])
    coef_out, extra_out = call(
        functools.partial(last_kernel, s),
        (f32(count * rows, lanes), f32(count * rows, lanes)),
        (base, inverse, coef, below_x, below_y), [], "last", 1_000_000)
    return (coef_out.reshape(signal.shape), extra_out.reshape(signal.shape), grad_out, sign_out)


def solution(mesh):
    cube = P(None, "gx", "gy", None)
    in_specs = (cube, P(), P(), P("gx", "gy", None), cube, cube, P(None, None, "gx", "gy", None), cube)
    out_specs = (cube, cube, P(None, None, "gx", "gy", None), cube)
    return jax.shard_map(per_device, mesh=mesh, in_specs=in_specs, out_specs=out_specs, check_vma=False)
```

```python
import functools

import jax
import jax.numpy as jnp
from jax import lax
from jax.experimental import pallas as pl
from jax.experimental.pallas import tpu as pltpu
from jax.sharding import PartitionSpec as P

STEP_PRIMAL = 0.25
STEP_DUAL = 0.02
TV_WEIGHT = 0.5

F32 = jnp.float32
BF16 = jnp.bfloat16
VMEM_LIMIT = 24 * 1024 * 1024
GROUP = 16
LANES = 128


def round_up(value, unit):
    return -(-value // unit) * unit


def split_two(value):
    high = value.astype(BF16)
    low = (value - high.astype(F32)).astype(BF16)
    return high, low


def put_cat(cat_ref, value, low_row):
    rows, width = value.shape
    high, low = split_two(value)
    cat_ref[0:rows, 0:width] = high
    cat_ref[rows : 2 * rows, 0:width] = high
    cat_ref[low_row : low_row + rows, 0:width] = low


def planes_of(ref, count, rows, padded):
    parts = []
    for row in range(rows):
        part = ref[pl.ds(row, count, stride=rows), :]
        parts.append(jnp.concatenate([part, jnp.zeros((padded - count, part.shape[1]), F32)], 0))
    return jnp.concatenate(parts, 1)


def matmul(left, right):
    return jnp.dot(left, right, preferred_element_type=F32)


def wide_matmul(left_ref, right_ref, out_ref, width):
    for start in range(0, width, 256):
        size = min(256, width - start)
        out_ref[:, start : start + size] = matmul(left_ref[...], right_ref[:, start : start + size])


def harmonics(adjoint_ref, high_ref, low_ref, start, size, padded):
    first = matmul(adjoint_ref[...], high_ref[:, start : start + size])
    second = matmul(adjoint_ref[0:padded, :], low_ref[:, start : start + size])
    return first[0:padded] + first[padded : 2 * padded] + second


def all_harmonics(adjoint_ref, high_ref, low_ref, width, padded):
    parts = [
        harmonics(adjoint_ref, high_ref, low_ref, start, min(256, width - start), padded)
        for start in range(0, width, 256)
    ]
    return jnp.concatenate(parts, 1)


def last_flags():
    last_x = lax.axis_index("gx") == lax.axis_size("gx") - 1
    last_y = lax.axis_index("gy") == lax.axis_size("gy") - 1
    keep_x = jnp.where(last_x, 0.0, 1.0).astype(F32)
    keep_y = jnp.where(last_y, 0.0, 1.0).astype(F32)
    return keep_x, keep_y


def lane_edge():
    lane = lax.broadcasted_iota(jnp.int32, (GROUP, LANES), 1)
    return jnp.where(lane == LANES - 1, 0.0, 1.0).astype(F32)


def shrunk(step_x, step_y, step_z):
    square = step_x * step_x + step_y * step_y + step_z * step_z
    factor = TV_WEIGHT * lax.rsqrt(jnp.maximum(square, TV_WEIGHT * TV_WEIGHT))
    return step_x * factor, step_y * factor, step_z * factor


def next_lane(value):
    return pltpu.roll(value, LANES - 1, 1)


def previous_lane(value):
    return pltpu.roll(value, 1, 1)


class Shape:
    def __init__(self, directions, count, rows, lanes):
        assert lanes == LANES
        self.directions, self.count, self.rows = directions, count, rows
        self.padded_dirs = round_up(directions, GROUP)
        self.padded = round_up(count + 1, GROUP)
        self.width = rows * lanes
        self.low_row = round_up(2 * self.padded, LANES)
        self.depth = self.low_row + self.padded
        self.groups = self.padded_dirs // GROUP
        self.part_rows = (rows + 1) * self.padded_dirs + 8

    def start(self, part, row):
        return part * self.part_rows + (row + 1) * self.padded_dirs

    def at(self, part, row, index):
        return pl.ds(pl.multiple_of(self.start(part, row) + index * GROUP, 8), GROUP)

    def lanes(self, row):
        return pl.ds(pl.multiple_of(row * LANES, LANES), LANES)


def load_kernel(s, e_ref, basis_ref, response_ref, grad_ref, sign_ref,
                dual_ref, sign_out, own_ref, cat_ref, adjoint_ref, column_ref,
                basis_in, response_in, padded_ref, e_cat, amp, sems):
    first = [
        pltpu.make_async_copy(basis_ref, basis_in, sems.at[4 * s.rows]),
        pltpu.make_async_copy(response_ref, response_in, sems.at[4 * s.rows + 1]),
        pltpu.make_async_copy(e_ref, own_ref, sems.at[4 * s.rows + 2]),
    ]
    for copy in first:
        copy.start()
    pad_rows = s.padded_dirs - s.directions
    for part in range(4):
        for row in range(s.rows):
            if pad_rows:
                end = s.start(part % 3, row) + s.padded_dirs
                place = sign_out if part == 3 else dual_ref
                place[end - pad_rows : end, :] = jnp.zeros((pad_rows, LANES), F32)

    def copy_of(part, row):
        source = sign_ref.at[:, 0, row] if part == 3 else grad_ref.at[part, :, 0, row]
        place = sign_out if part == 3 else dual_ref
        target = place.at[pl.ds(s.start(part % 3, row), s.directions)]
        return pltpu.make_async_copy(source, target, sems.at[part * s.rows + row])

    for row in range(s.rows):
        for part in (1, 2, 3):
            copy_of(part, row).start()
    for row in range(s.rows):
        copy_of(0, row).start()

    padded_ref[...] = jnp.zeros_like(padded_ref)
    for copy in first:
        copy.wait()
    padded_ref[0 : s.count, 0 : s.directions] = basis_in[...]
    whole = padded_ref[...]
    high, low = split_two(whole)
    adjoint_ref[0 : s.padded, :] = high[0 : s.padded, 0 : s.padded_dirs]
    adjoint_ref[s.padded : 2 * s.padded, :] = low[0 : s.padded, 0 : s.padded_dirs]
    high = high.astype(F32).T[0 : s.padded_dirs]
    low = low.astype(F32).T[0 : s.padded_dirs]
    cat_ref[:, 0:LANES] = (high + pltpu.roll(low, s.padded, 1)).astype(BF16)
    cat_ref[:, s.low_row : s.low_row + s.padded] = high[:, 0 : s.padded].astype(BF16)
    row_index = lax.broadcasted_iota(jnp.int32, (s.padded, LANES), 0)
    lane_index = lax.broadcasted_iota(jnp.int32, (s.padded, LANES), 1)
    spread = jnp.concatenate([response_in[...], jnp.zeros((1, LANES - s.count), F32)], 1)
    picked = jnp.where(row_index == lane_index, spread, 0.0)
    column_ref[...] = jnp.broadcast_to(jnp.sum(picked, 1, keepdims=True), (s.padded, LANES))

    e_cat[...] = jnp.zeros_like(e_cat)
    put_cat(e_cat, planes_of(own_ref, s.count, s.rows, s.padded) * STEP_DUAL, s.low_row)
    wide_matmul(cat_ref, e_cat, amp, s.width)
    edge = lane_edge()

    def update_row(row):
        for part in (1, 2, 3):
            copy_of(part, row).wait()
        for index in range(s.groups):
            here = slice(index * GROUP, (index + 1) * GROUP)
            value = amp[here, s.lanes(row)]
            if not isinstance(row, int):
                dual_ref[s.at(1, row, index), :] += amp[here, s.lanes(row + 1)] - value
            dual_ref[s.at(2, row, index), :] += (next_lane(value) - value) * edge
            sign = sign_out[s.at(0, row, index), :] + value
            sign_out[s.at(0, row, index), :] = jnp.minimum(0.0, sign)

    def step(row, carry):
        update_row(row)
        return carry

    lax.fori_loop(0, s.rows - 1, step, 0)
    update_row(s.rows - 1)
    for row in range(s.rows):
        copy_of(0, row).wait()


def dual_pass(s, dual_in, sign_in, dual_out, sign_out, change, highs):
    edge = lane_edge()
    back_high, back_low, x_high, x_low, y_high, y_low = highs
    full = sign_out is not None
    signs = sign_out if full else sign_in
    dual_out[s.start(1, -1) : s.start(1, 0), :] = jnp.zeros((s.padded_dirs, LANES), F32)

    def part_lanes(part, row):
        return pl.ds(pl.multiple_of(part * s.width + row * LANES, LANES), LANES)

    def shrink_row(row):
        for index in range(s.groups):
            here = slice(index * GROUP, (index + 1) * GROUP)
            step_x = dual_in[s.at(0, row, index), :] + change[here, part_lanes(0, row)]
            step_y, step_z = dual_in[s.at(1, row, index), :], dual_in[s.at(2, row, index), :]
            if full:
                step_y = step_y + change[here, part_lanes(1, row)]
                step_z = step_z + change[here, part_lanes(2, row)]
                sign_out[s.at(0, row, index), :] = jnp.minimum(
                    0.0, sign_in[s.at(0, row, index), :] + change[here, part_lanes(3, row)])
            elif isinstance(row, int):
                step_y = step_y + change[here, part_lanes(1, 0)]
            new_x, new_y, new_z = shrunk(step_x, step_y, step_z)
            dual_out[s.at(0, row, index), :] = new_x
            dual_out[s.at(1, row, index), :] = new_y
            dual_out[s.at(2, row, index), :] = new_z

    def split_row(row, carry):
        for index in range(s.groups):
            here = slice(index * GROUP, (index + 1) * GROUP)
            inner_z = dual_out[s.at(2, row, index), :] * edge
            back = signs[s.at(0, row, index), :] - (inner_z - previous_lane(inner_z))
            back = back - (dual_out[s.at(1, row, index), :] - dual_out[s.at(1, row - 1, index), :])
            back_high[here, s.lanes(row)], back_low[here, s.lanes(row)] = split_two(back)
            x_high[here, s.lanes(row)], x_low[here, s.lanes(row)] = split_two(
                dual_out[s.at(0, row, index), :])
        return carry

    def step(row, carry):
        shrink_row(row)
        return carry

    if full:
        lax.fori_loop(0, s.rows, step, 0)
    else:
        lax.fori_loop(0, s.rows - 1, step, 0)
        shrink_row(s.rows - 1)
    lax.fori_loop(0, s.rows, split_row, 0)
    for index in range(s.groups):
        here = slice(index * GROUP, (index + 1) * GROUP)
        y_high[here, :], y_low[here, :] = split_two(dual_out[s.at(1, s.rows - 1, index), :])


def all_adjoints(s, adjoint_ref, splits, keep_x, keep_y):
    back_high, back_low, x_high, x_low, y_high, y_low = splits
    from_back = all_harmonics(adjoint_ref, back_high, back_low, s.width, s.padded)
    from_x = all_harmonics(adjoint_ref, x_high, x_low, s.width, s.padded)
    from_y = all_harmonics(adjoint_ref, y_high, y_low, LANES, s.padded)
    last = from_back[:, s.width - LANES :] + (1.0 - keep_y) * from_y
    total = jnp.concatenate([from_back[:, : s.width - LANES], last], 1) - keep_x * from_x
    return total, from_x, from_y


def weights(s, mask_ref, response_ref):
    mask = jnp.concatenate(
        [mask_ref[row : row + 1, :].astype(F32) for row in range(s.rows)], 1)
    return mask, jnp.concatenate([response_ref[...]] * s.rows, 1)


def is_odd(axis):
    return lax.rem(lax.axis_index(axis), 2) == 1


def to_partners(axis, upward, downward):
    odd = jnp.broadcast_to(is_odd(axis), upward.shape)
    return jnp.where(odd, downward, upward), jnp.where(odd, upward, downward)


def from_partners(axis, over_even, over_odd):
    if over_odd is None:
        over_odd = jnp.zeros_like(over_even)
    odd = jnp.broadcast_to(is_odd(axis), over_even.shape)
    return jnp.where(odd, over_even, over_odd), jnp.where(odd, over_odd, over_even)


def received_at(axis, refs):
    return from_partners(axis, refs[0][...], refs[1][...] if len(refs) > 1 else None)


def first_kernel(s, dual_in, sign_in, cat_ref, adjoint_ref, e_ref, ex_ref, coef_ref, signal_ref,
                 mask_ref, response_ref, *refs):
    pairs_y = len(pair_lists(lax.axis_size("gy")))
    received, refs = refs[:pairs_y], refs[pairs_y:]
    dual_ref, base_ref, inverse_ref, coef_out, target_ref, x_ref, y_ref, *send_refs = refs[:-8]
    e_cat, diff = refs[-8:-6]
    keep_x, keep_y = last_flags()
    here = planes_of(e_ref, s.count, s.rows, s.padded)
    there = planes_of(ex_ref, s.count, s.rows, s.padded)
    _, edge_row = received_at("gy", received)
    edge_row = jnp.concatenate([edge_row, jnp.zeros((s.padded - s.count, LANES), F32)], 0)
    e_cat[2 * s.padded : s.low_row, :] = jnp.zeros((s.low_row - 2 * s.padded, s.width + LANES), BF16)
    put_cat(e_cat, jnp.concatenate(
        [(there - here) * (STEP_DUAL * keep_x),
         (edge_row - here[:, s.width - LANES :]) * (STEP_DUAL * keep_y)], 1), s.low_row)
    wide_matmul(cat_ref, e_cat, diff, s.width + LANES)
    dual_pass(s, dual_in, sign_in, dual_ref, None, diff, refs[-6:])
    total, from_x, from_y = all_adjoints(s, adjoint_ref, refs[-6:], keep_x, keep_y)
    mask, response = weights(s, mask_ref, response_ref)
    weight = mask * response
    coef = planes_of(coef_ref, s.count, s.rows, s.padded)
    signal = planes_of(signal_ref, s.count, s.rows, s.padded)
    target = STEP_PRIMAL * weight * signal
    inverse = 1.0 / (1.0 + STEP_PRIMAL * weight * response)
    base = coef + target - STEP_PRIMAL * total
    row_index = lax.broadcasted_iota(jnp.int32, (s.padded, s.width), 0)
    ahead = jnp.where(row_index == s.count, mask, 2.0 * base * inverse - coef)
    base_ref[...] = base
    inverse_ref[...] = inverse
    coef_out[...] = coef
    target_ref[...] = target
    x_ref[...] = from_x
    y_ref[...] = from_y
    messages = (
        to_partners("gx", from_x, ahead) + to_partners("gy", from_y, ahead[:, 0:LANES])[:pairs_y]
        + to_partners("gy", from_y, from_x[:, 0:LANES])[:pairs_y])
    for send_ref, message in zip(send_refs, messages):
        send_ref[...] = message


def add_first_row(planes, row):
    return jnp.concatenate([planes[:, 0:LANES] + row, planes[:, LANES:]], 1)


def ahead_of(s, message, own, response):
    row_index = lax.broadcasted_iota(jnp.int32, message.shape, 0)
    mask = message[s.count : s.count + 1, :]
    inverse = 1.0 / (1.0 + STEP_PRIMAL * (mask * response) * response)
    return jnp.where(row_index < s.count, message - (2.0 * STEP_PRIMAL) * inverse * own, 0.0)


def second_kernel(s, dual_in, sign_in, cat_ref, adjoint_ref, base_ref, inverse_ref, coef_ref, target_ref,
                  x_ref, y_ref, response_ref, *refs):
    *received, dual_ref, sign_ref, base_out, coef_out, x_out, y_out = refs[:-8]
    e_cat, change, *splits = refs[-8:]
    pairs_y = (len(received) - 2) // 2
    keep_x, keep_y = last_flags()
    below, above = received_at("gx", received[:2])
    below_y, above_y = received_at("gy", received[2 : 2 + pairs_y])
    below_d, above_d = received_at("gy", received[2 + pairs_y :])
    response = response_ref[...]
    coef = coef_ref[...]
    updated = (base_ref[...] - STEP_PRIMAL * add_first_row(below, below_y)) * inverse_ref[...]
    here = 2.0 * updated - coef
    wide = jnp.concatenate([response] * s.rows, 1)
    there = ahead_of(s, above, add_first_row(x_ref[...], below_d), wide)
    edge_row = ahead_of(s, above_y, y_ref[...] + above_d, response)
    e_cat[2 * s.padded : s.low_row, :] = jnp.zeros((s.low_row - 2 * s.padded, 4 * s.width), BF16)
    edge = lane_edge()[0:1]
    planes = [here[:, row * LANES : (row + 1) * LANES] for row in range(s.rows)]
    along_y = jnp.concatenate([here[:, LANES:], edge_row], 1) - here
    along_y = jnp.concatenate(
        [along_y[:, : s.width - LANES], keep_y * along_y[:, s.width - LANES :]], 1)
    along_z = jnp.concatenate([(next_lane(plane) - plane) * edge for plane in planes], 1)
    put_cat(e_cat, STEP_DUAL * jnp.concatenate(
        [(there - here) * keep_x, along_y, along_z, here], 1), s.low_row)
    wide_matmul(cat_ref, e_cat, change, 4 * s.width)
    dual_pass(s, dual_in, sign_in, dual_ref, sign_ref, change, splits)
    total, from_x, from_y = all_adjoints(s, adjoint_ref, splits, keep_x, keep_y)
    base_out[...] = updated + target_ref[...] - STEP_PRIMAL * total
    coef_out[...] = updated
    x_out[...] = from_x
    y_out[...] = from_y


def store_kernel(s, dual_ref, sign_in, grad_ref, sign_ref, sems):
    copies = []
    for row in range(s.rows):
        for part in range(3):
            copies.append(pltpu.make_async_copy(
                dual_ref.at[pl.ds(s.start(part, row), s.directions)], grad_ref.at[part, :, 0, row],
                sems.at[part * s.rows + row]))
        copies.append(pltpu.make_async_copy(
            sign_in.at[pl.ds(s.start(0, row), s.directions)], sign_ref.at[:, 0, row],
            sems.at[3 * s.rows + row]))
    for copy in copies:
        copy.start()
    for copy in copies:
        copy.wait()


def last_kernel(s, base_ref, inverse_ref, coef_ref, x_ref, *refs):
    *received, coef_out, extra_out = refs
    below_y, _ = received_at("gy", received)
    total = add_first_row(x_ref[...], below_y)
    updated = (base_ref[...] - STEP_PRIMAL * total) * inverse_ref[...]
    extra = 2.0 * updated - coef_ref[...]
    for row in range(s.rows):
        at = slice(row * LANES, (row + 1) * LANES)
        coef_out[pl.ds(row, s.count, stride=s.rows), :] = updated[0 : s.count, at]
        extra_out[pl.ds(row, s.count, stride=s.rows), :] = extra[0 : s.count, at]


def call(kernel, outs, ins, scratch, name, flops, in_specs=None, out_specs=None, aliases=None):
    vmem = pl.BlockSpec(memory_space=pltpu.VMEM)
    count = len(outs) if isinstance(outs, (tuple, list)) else 1
    size = lambda arrays: sum(a.size * a.dtype.itemsize for a in jax.tree.leaves(arrays))
    return pl.pallas_call(
        kernel,
        out_shape=outs,
        in_specs=in_specs or [vmem] * len(ins),
        out_specs=out_specs or ([vmem] * count if isinstance(outs, (tuple, list)) else vmem),
        scratch_shapes=scratch,
        input_output_aliases=aliases or {},
        compiler_params=pltpu.CompilerParams(vmem_limit_bytes=VMEM_LIMIT),
        cost_estimate=pl.CostEstimate(
            flops=flops, bytes_accessed=size(outs) + size(list(ins)), transcendentals=0),
        name=name,
    )(*ins)


def pair_lists(count):
    even = [pair for low in range(0, count - 1, 2) for pair in ((low, low + 1), (low + 1, low))]
    odd = [pair for low in range(1, count - 1, 2) for pair in ((low, low + 1), (low + 1, low))]
    return [even, odd] if odd else [even]


def exchange(axis, sends):
    lists = pair_lists(lax.axis_size(axis))
    return [lax.ppermute(send, axis, pairs) for send, pairs in zip(sends, lists)]


def diagonal_exchange(sends):
    count_x, count_y = lax.axis_size("gx"), lax.axis_size("gy")
    received = []
    for send, pairs in zip(sends, pair_lists(count_y)):
        flat = []
        for low, high in pairs:
            if low < high:
                for x in range(1, count_x):
                    ends = (x * count_y + low, (x - 1) * count_y + high)
                    flat += [ends, ends[::-1]]
        received.append(lax.ppermute(send, ("gx", "gy"), flat))
    return received


def shift(value, axis, steps):
    count = lax.axis_size(axis)
    pairs = [(i, i + steps) for i in range(count) if 0 <= i + steps < count]
    return lax.ppermute(value, axis, pairs)


def per_device(signal, response, basis, mask, coefficients, extrapolated, dual_grad, dual_sign):
    count, layers, rows, lanes = signal.shape
    assert layers == 1
    s = Shape(basis.shape[0], count, rows, lanes)
    flat = lambda a: a.reshape(count * rows, lanes)
    f32 = lambda *shape: jax.ShapeDtypeStruct(shape, F32)
    bf16 = lambda *shape: jax.ShapeDtypeStruct(shape, BF16)
    vmem = pl.BlockSpec(memory_space=pltpu.VMEM)
    hbm = pl.BlockSpec(memory_space=pltpu.HBM)
    dirs, padded, width = s.padded_dirs, s.padded, s.width
    splits = [pltpu.VMEM((dirs, width), BF16)] * 4 + [pltpu.VMEM((dirs, LANES), BF16)] * 2
    dual = f32(3 * s.part_rows, lanes)
    signs = f32(s.part_rows, lanes)
    plane = f32(padded, width)

    after_x = shift(extrapolated, "gx", -1)
    pairs_y = len(pair_lists(lax.axis_size("gy")))
    after_y = exchange("gy", [extrapolated[:, 0, 0]] * pairs_y)
    in_hbm = lambda a: pltpu.with_memory_space_constraint(a, pltpu.HBM)
    line = f32(padded, lanes)
    duals, sign, own, cat, adjoint, column = call(
        functools.partial(load_kernel, s),
        (dual, signs, f32(count * rows, lanes), bf16(dirs, s.depth), bf16(2 * padded, dirs), line),
        [in_hbm(a) for a in
         (flat(extrapolated), basis.T, response[None], dual_grad, dual_sign)],
        [pltpu.VMEM((count, s.directions), F32), pltpu.VMEM((1, count), F32),
         pltpu.VMEM((LANES, round_up(dirs, LANES)), F32), pltpu.VMEM((s.depth, width), BF16),
         pltpu.VMEM((dirs, width), F32), pltpu.SemaphoreType.DMA((4 * rows + 3,))],
        "load", 2_000_000_000, in_specs=[hbm] * 5)
    duals, base, inverse, coef, target, from_x, from_y, *sends = call(
        functools.partial(first_kernel, s),
        (dual,) + (plane,) * 5 + (line,) + (plane,) * 2 + (line,) * (2 * pairs_y),
        [duals, sign, cat, adjoint, own, flat(after_x), flat(coefficients), flat(signal),
         mask[0], column] + after_y,
        [pltpu.VMEM((s.depth, width + LANES), BF16), pltpu.VMEM((dirs, width + LANES), F32)] + splits,
        "first", 2_000_000_000)
    received = exchange("gx", sends[:2])
    received += exchange("gy", sends[2 : 2 + pairs_y]) + diagonal_exchange(sends[2 + pairs_y :])
    duals, sign, base, coef, from_x, from_y = call(
        functools.partial(second_kernel, s),
        (dual, signs, plane, plane, plane, line),
        [duals, sign, cat, adjoint, base, inverse, coef, target, from_x, from_y, column] + received,
        [pltpu.VMEM((s.depth, 4 * width), BF16), pltpu.VMEM((dirs, 4 * width), F32)] + splits,
        "second", 2_000_000_000)
    below_x = shift(from_x, "gx", 1)
    below_y = exchange("gy", [from_y] * pairs_y)
    grad_out, sign_out = call(
        functools.partial(store_kernel, s),
        (f32(*dual_grad.shape), f32(*dual_sign.shape)), (duals, sign),
        [pltpu.SemaphoreType.DMA((4 * rows,))], "store", 2_000_000_000, out_specs=[hbm, hbm])
    coef_out, extra_out = call(
        functools.partial(last_kernel, s),
        (f32(count * rows, lanes), f32(count * rows, lanes)),
        [base, inverse, coef, below_x] + below_y, [], "last", 1_000_000)
    return (coef_out.reshape(signal.shape), extra_out.reshape(signal.shape), grad_out, sign_out)


def solution(mesh):
    cube = P(None, "gx", "gy", None)
    in_specs = (cube, P(), P(), P("gx", "gy", None), cube, cube, P(None, None, "gx", "gy", None), cube)
    out_specs = (cube, cube, P(None, None, "gx", "gy", None), cube)
    return jax.shard_map(per_device, mesh=mesh, in_specs=in_specs, out_specs=out_specs, check_vma=False)
```

```python
import functools

import jax
import jax.numpy as jnp
from jax import lax
from jax.experimental import pallas as pl
from jax.experimental.pallas import tpu as pltpu
from jax.sharding import PartitionSpec as P


STEP_PRIMAL = 0.25
STEP_DUAL = 0.02
TV_WEIGHT = 0.5

F32 = jnp.float32
BF16 = jnp.bfloat16
VMEM_LIMIT = 24 * 1024 * 1024
GROUP = 16
LANES = 128


def round_up(value, unit):
    return -(-value // unit) * unit


def split_two(value):
    high = value.astype(BF16)
    low = (value - high.astype(F32)).astype(BF16)
    return high, low


def put_cat(cat_ref, value, low_row):
    rows, width = value.shape
    high, low = split_two(value)
    cat_ref[0:rows, 0:width] = high
    cat_ref[rows : 2 * rows, 0:width] = high
    cat_ref[low_row : low_row + rows, 0:width] = low


def planes_of(ref, count, rows, padded):
    parts = []
    for row in range(rows):
        part = ref[pl.ds(row, count, stride=rows), :]
        parts.append(jnp.concatenate([part, jnp.zeros((padded - count, part.shape[1]), F32)], 0))
    return jnp.concatenate(parts, 1)


def matmul(left, right):
    return jnp.dot(left, right, preferred_element_type=F32)


def wide_matmul(left_ref, right_ref, out_ref, width):
    for start in range(0, width, 256):
        size = min(256, width - start)
        out_ref[:, start : start + size] = matmul(left_ref[...], right_ref[:, start : start + size])


def harmonics(adjoint_ref, value, padded):
    high, low = split_two(value)
    first = matmul(adjoint_ref[...], high)
    second = matmul(adjoint_ref[0:padded, :], low)
    return first[0:padded] + first[padded : 2 * padded] + second


def last_flags():
    last_x = lax.axis_index("gx") == lax.axis_size("gx") - 1
    last_y = lax.axis_index("gy") == lax.axis_size("gy") - 1
    keep_x = jnp.where(last_x, 0.0, 1.0).astype(F32)
    keep_y = jnp.where(last_y, 0.0, 1.0).astype(F32)
    return keep_x, keep_y


def lane_edge():
    lane = lax.broadcasted_iota(jnp.int32, (GROUP, LANES), 1)
    return jnp.where(lane == LANES - 1, 0.0, 1.0).astype(F32)


def shrunk(step_x, step_y, step_z):
    square = step_x * step_x + step_y * step_y + step_z * step_z
    factor = TV_WEIGHT * lax.rsqrt(jnp.maximum(square, TV_WEIGHT * TV_WEIGHT))
    return step_x * factor, step_y * factor, step_z * factor


def next_lane(value):
    return pltpu.roll(value, LANES - 1, 1)


def previous_lane(value):
    return pltpu.roll(value, 1, 1)


class Shape:
    def __init__(self, directions, count, rows, lanes):
        assert lanes == LANES
        self.directions, self.count, self.rows = directions, count, rows
        self.padded_dirs = round_up(directions, GROUP)
        self.padded = round_up(count + 1, GROUP)
        self.width = rows * lanes
        self.low_row = round_up(2 * self.padded, LANES)
        self.depth = self.low_row + self.padded
        self.groups = self.padded_dirs // GROUP
        self.part_rows = (rows + 1) * self.padded_dirs + 8

    def start(self, part, row):
        return part * self.part_rows + (row + 1) * self.padded_dirs

    def at(self, part, row, index):
        return pl.ds(pl.multiple_of(self.start(part, row) + index * GROUP, 8), GROUP)

    def lanes(self, row):
        return pl.ds(pl.multiple_of(row * LANES, LANES), LANES)


def load_kernel(s, e_ref, basis_ref, response_ref, grad_ref, sign_ref,
                dual_ref, sign_out, own_ref, cat_ref, adjoint_ref, column_ref,
                basis_in, response_in, padded_ref, e_cat, amp, sems):
    first = [
        pltpu.make_async_copy(basis_ref, basis_in, sems.at[4 * s.rows]),
        pltpu.make_async_copy(response_ref, response_in, sems.at[4 * s.rows + 1]),
        pltpu.make_async_copy(e_ref, own_ref, sems.at[4 * s.rows + 2]),
    ]
    for copy in first:
        copy.start()
    pad_rows = s.padded_dirs - s.directions
    for part in range(4):
        for row in range(s.rows):
            if pad_rows:
                end = s.start(part % 3, row) + s.padded_dirs
                place = sign_out if part == 3 else dual_ref
                place[end - pad_rows : end, :] = jnp.zeros((pad_rows, LANES), F32)

    def copy_of(part, row):
        source = sign_ref.at[:, 0, row] if part == 3 else grad_ref.at[part, :, 0, row]
        place = sign_out if part == 3 else dual_ref
        target = place.at[pl.ds(s.start(part % 3, row), s.directions)]
        return pltpu.make_async_copy(source, target, sems.at[part * s.rows + row])

    for row in range(s.rows):
        for part in (1, 2, 3):
            copy_of(part, row).start()
    for row in range(s.rows):
        copy_of(0, row).start()

    padded_ref[...] = jnp.zeros_like(padded_ref)
    for copy in first:
        copy.wait()
    padded_ref[0 : s.count, 0 : s.directions] = basis_in[...]
    whole = padded_ref[...]
    high, low = split_two(whole)
    adjoint_ref[0 : s.padded, :] = high[0 : s.padded, 0 : s.padded_dirs]
    adjoint_ref[s.padded : 2 * s.padded, :] = low[0 : s.padded, 0 : s.padded_dirs]
    high = high.astype(F32).T[0 : s.padded_dirs]
    low = low.astype(F32).T[0 : s.padded_dirs]
    cat_ref[:, 0:LANES] = (high + pltpu.roll(low, s.padded, 1)).astype(BF16)
    cat_ref[:, s.low_row : s.low_row + s.padded] = high[:, 0 : s.padded].astype(BF16)
    row_index = lax.broadcasted_iota(jnp.int32, (s.padded, LANES), 0)
    lane_index = lax.broadcasted_iota(jnp.int32, (s.padded, LANES), 1)
    spread = jnp.concatenate([response_in[...], jnp.zeros((1, LANES - s.count), F32)], 1)
    picked = jnp.where(row_index == lane_index, spread, 0.0)
    column_ref[...] = jnp.broadcast_to(jnp.sum(picked, 1, keepdims=True), (s.padded, LANES))

    e_cat[...] = jnp.zeros_like(e_cat)
    put_cat(e_cat, planes_of(own_ref, s.count, s.rows, s.padded) * STEP_DUAL, s.low_row)
    wide_matmul(cat_ref, e_cat, amp, s.width)
    edge = lane_edge()

    def update_row(row):
        for part in (1, 2, 3):
            copy_of(part, row).wait()
        for index in range(s.groups):
            here = slice(index * GROUP, (index + 1) * GROUP)
            value = amp[here, s.lanes(row)]
            if not isinstance(row, int):
                dual_ref[s.at(1, row, index), :] += amp[here, s.lanes(row + 1)] - value
            dual_ref[s.at(2, row, index), :] += (next_lane(value) - value) * edge
            sign = sign_out[s.at(0, row, index), :] + value
            sign_out[s.at(0, row, index), :] = jnp.minimum(0.0, sign)

    def step(row, carry):
        update_row(row)
        return carry

    lax.fori_loop(0, s.rows - 1, step, 0)
    update_row(s.rows - 1)
    for row in range(s.rows):
        copy_of(0, row).wait()


def dual_pass(s, dual_in, sign_in, dual_out, sign_out, change, back_ref):
    edge = lane_edge()
    full = sign_out is not None
    signs = sign_out if full else sign_in
    dual_out[s.start(1, -1) : s.start(1, 0), :] = jnp.zeros((s.padded_dirs, LANES), F32)

    def part_lanes(part, row):
        return pl.ds(pl.multiple_of(part * s.width + row * LANES, LANES), LANES)

    def shrink_row(row):
        for index in range(s.groups):
            here = slice(index * GROUP, (index + 1) * GROUP)
            step_x = dual_in[s.at(0, row, index), :] + change[here, part_lanes(0, row)]
            step_y, step_z = dual_in[s.at(1, row, index), :], dual_in[s.at(2, row, index), :]
            if full:
                step_y = step_y + change[here, part_lanes(1, row)]
                step_z = step_z + change[here, part_lanes(2, row)]
                sign_out[s.at(0, row, index), :] = jnp.minimum(
                    0.0, sign_in[s.at(0, row, index), :] + change[here, part_lanes(3, row)])
            elif isinstance(row, int):
                step_y = step_y + change[here, part_lanes(1, 0)]
            new_x, new_y, new_z = shrunk(step_x, step_y, step_z)
            dual_out[s.at(0, row, index), :] = new_x
            dual_out[s.at(1, row, index), :] = new_y
            dual_out[s.at(2, row, index), :] = new_z

    def split_row(row, carry):
        for index in range(s.groups):
            here = slice(index * GROUP, (index + 1) * GROUP)
            inner_z = dual_out[s.at(2, row, index), :] * edge
            back = signs[s.at(0, row, index), :] - (inner_z - previous_lane(inner_z))
            back = back - (dual_out[s.at(1, row, index), :] - dual_out[s.at(1, row - 1, index), :])
            back_ref[here, s.lanes(row)] = back
        return carry

    def step(row, carry):
        shrink_row(row)
        return carry

    if full:
        lax.fori_loop(0, s.rows, step, 0)
    else:
        lax.fori_loop(0, s.rows - 1, step, 0)
        shrink_row(s.rows - 1)
    lax.fori_loop(0, s.rows, split_row, 0)


def all_adjoints(s, adjoint_ref, back_ref, dual_ref, keep_x, keep_y):
    def plane(part, row):
        return dual_ref[pl.ds(s.start(part, row), s.padded_dirs), :]

    from_back, from_x = [], []
    for row in range(0, s.rows, 2):
        rows = range(row, min(row + 2, s.rows))
        value = back_ref[:, row * LANES : (row + len(rows)) * LANES]
        from_back.append(harmonics(adjoint_ref, value, s.padded))
        value = jnp.concatenate([plane(0, each) for each in rows], 1)
        from_x.append(harmonics(adjoint_ref, value, s.padded))
    from_back, from_x = jnp.concatenate(from_back, 1), jnp.concatenate(from_x, 1)
    from_y = harmonics(adjoint_ref, plane(1, s.rows - 1), s.padded)
    last = from_back[:, s.width - LANES :] + (1.0 - keep_y) * from_y
    total = jnp.concatenate([from_back[:, : s.width - LANES], last], 1) - keep_x * from_x
    return total, from_x, from_y


def weights(s, mask_ref, response_ref):
    mask = jnp.concatenate(
        [mask_ref[row : row + 1, :].astype(F32) for row in range(s.rows)], 1)
    return mask, jnp.concatenate([response_ref[...]] * s.rows, 1)


def is_odd(axis):
    return lax.rem(lax.axis_index(axis), 2) == 1


def to_partners(axis, upward, downward):
    odd = jnp.broadcast_to(is_odd(axis), upward.shape)
    return jnp.where(odd, downward, upward), jnp.where(odd, upward, downward)


def from_partners(axis, over_even, over_odd):
    if over_odd is None:
        over_odd = jnp.zeros_like(over_even)
    odd = jnp.broadcast_to(is_odd(axis), over_even.shape)
    return jnp.where(odd, over_even, over_odd), jnp.where(odd, over_odd, over_even)


def received_at(axis, refs):
    return from_partners(axis, refs[0][...], refs[1][...] if len(refs) > 1 else None)


def first_kernel(s, dual_in, sign_in, cat_ref, adjoint_ref, e_ref, ex_ref, coef_ref, signal_ref,
                 mask_ref, response_ref, *refs):
    pairs_y = len(pair_lists(lax.axis_size("gy")))
    received, refs = refs[:pairs_y], refs[pairs_y:]
    dual_ref, base_ref, inverse_ref, coef_out, target_ref, x_ref, y_ref, *send_refs = refs[:-3]
    e_cat, diff, back_ref = refs[-3:]
    keep_x, keep_y = last_flags()
    here = planes_of(e_ref, s.count, s.rows, s.padded)
    there = planes_of(ex_ref, s.count, s.rows, s.padded)
    _, edge_row = received_at("gy", received)
    edge_row = jnp.concatenate([edge_row, jnp.zeros((s.padded - s.count, LANES), F32)], 0)
    e_cat[2 * s.padded : s.low_row, :] = jnp.zeros((s.low_row - 2 * s.padded, s.width + LANES), BF16)
    put_cat(e_cat, jnp.concatenate(
        [(there - here) * (STEP_DUAL * keep_x),
         (edge_row - here[:, s.width - LANES :]) * (STEP_DUAL * keep_y)], 1), s.low_row)
    wide_matmul(cat_ref, e_cat, diff, s.width + LANES)
    dual_pass(s, dual_in, sign_in, dual_ref, None, diff, back_ref)
    total, from_x, from_y = all_adjoints(s, adjoint_ref, back_ref, dual_ref, keep_x, keep_y)
    mask, response = weights(s, mask_ref, response_ref)
    weight = mask * response
    coef = planes_of(coef_ref, s.count, s.rows, s.padded)
    signal = planes_of(signal_ref, s.count, s.rows, s.padded)
    target = STEP_PRIMAL * weight * signal
    inverse = 1.0 / (1.0 + STEP_PRIMAL * weight * response)
    base = coef + target - STEP_PRIMAL * total
    row_index = lax.broadcasted_iota(jnp.int32, (s.padded, s.width), 0)
    ahead = jnp.where(row_index == s.count, mask, 2.0 * base * inverse - coef)
    base_ref[...] = base
    inverse_ref[...] = inverse
    coef_out[...] = coef
    target_ref[...] = target
    x_ref[...] = from_x
    y_ref[...] = from_y
    messages = (
        to_partners("gx", from_x, ahead) + to_partners("gy", from_y, ahead[:, 0:LANES])[:pairs_y]
        + to_partners("gy", from_y, from_x[:, 0:LANES])[:pairs_y])
    for send_ref, message in zip(send_refs, messages):
        send_ref[...] = message


def add_first_row(planes, row):
    return jnp.concatenate([planes[:, 0:LANES] + row, planes[:, LANES:]], 1)


def ahead_of(s, message, own, response):
    row_index = lax.broadcasted_iota(jnp.int32, message.shape, 0)
    mask = message[s.count : s.count + 1, :]
    inverse = 1.0 / (1.0 + STEP_PRIMAL * (mask * response) * response)
    return jnp.where(row_index < s.count, message - (2.0 * STEP_PRIMAL) * inverse * own, 0.0)


def second_kernel(s, dual_in, sign_in, cat_ref, adjoint_ref, base_ref, inverse_ref, coef_ref, target_ref,
                  x_ref, y_ref, response_ref, *refs):
    *received, dual_ref, sign_ref, base_out, coef_out, x_out, y_out = refs[:-3]
    e_cat, change, back_ref = refs[-3:]
    pairs_y = (len(received) - 2) // 2
    keep_x, keep_y = last_flags()
    below, above = received_at("gx", received[:2])
    below_y, above_y = received_at("gy", received[2 : 2 + pairs_y])
    below_d, above_d = received_at("gy", received[2 + pairs_y :])
    response = response_ref[...]
    coef = coef_ref[...]
    updated = (base_ref[...] - STEP_PRIMAL * add_first_row(below, below_y)) * inverse_ref[...]
    here = 2.0 * updated - coef
    wide = jnp.concatenate([response] * s.rows, 1)
    there = ahead_of(s, above, add_first_row(x_ref[...], below_d), wide)
    edge_row = ahead_of(s, above_y, y_ref[...] + above_d, response)
    e_cat[2 * s.padded : s.low_row, :] = jnp.zeros((s.low_row - 2 * s.padded, 4 * s.width), BF16)
    edge = lane_edge()[0:1]
    planes = [here[:, row * LANES : (row + 1) * LANES] for row in range(s.rows)]
    along_y = jnp.concatenate([here[:, LANES:], edge_row], 1) - here
    along_y = jnp.concatenate(
        [along_y[:, : s.width - LANES], keep_y * along_y[:, s.width - LANES :]], 1)
    along_z = jnp.concatenate([(next_lane(plane) - plane) * edge for plane in planes], 1)
    put_cat(e_cat, STEP_DUAL * jnp.concatenate(
        [(there - here) * keep_x, along_y, along_z, here], 1), s.low_row)
    wide_matmul(cat_ref, e_cat, change, 4 * s.width)
    dual_pass(s, dual_in, sign_in, dual_ref, sign_ref, change, back_ref)
    total, from_x, from_y = all_adjoints(s, adjoint_ref, back_ref, dual_ref, keep_x, keep_y)
    base_out[...] = updated + target_ref[...] - STEP_PRIMAL * total
    coef_out[...] = updated
    x_out[...] = from_x
    y_out[...] = from_y


def store_kernel(s, dual_ref, sign_in, grad_ref, sign_ref, sems):
    copies = []
    for row in range(s.rows):
        for part in range(3):
            copies.append(pltpu.make_async_copy(
                dual_ref.at[pl.ds(s.start(part, row), s.directions)], grad_ref.at[part, :, 0, row],
                sems.at[part * s.rows + row]))
        copies.append(pltpu.make_async_copy(
            sign_in.at[pl.ds(s.start(0, row), s.directions)], sign_ref.at[:, 0, row],
            sems.at[3 * s.rows + row]))
    for copy in copies:
        copy.start()
    for copy in copies:
        copy.wait()


def last_kernel(s, base_ref, inverse_ref, coef_ref, x_ref, *refs):
    *received, coef_out, extra_out = refs
    below_y, _ = received_at("gy", received)
    total = add_first_row(x_ref[...], below_y)
    updated = (base_ref[...] - STEP_PRIMAL * total) * inverse_ref[...]
    extra = 2.0 * updated - coef_ref[...]
    for row in range(s.rows):
        at = slice(row * LANES, (row + 1) * LANES)
        coef_out[pl.ds(row, s.count, stride=s.rows), :] = updated[0 : s.count, at]
        extra_out[pl.ds(row, s.count, stride=s.rows), :] = extra[0 : s.count, at]


def call(kernel, outs, ins, scratch, flops, in_specs=None, out_specs=None, aliases=None):
    vmem = pl.BlockSpec(memory_space=pltpu.VMEM)
    count = len(outs) if isinstance(outs, (tuple, list)) else 1
    size = lambda arrays: sum(a.size * a.dtype.itemsize for a in jax.tree.leaves(arrays))
    return pl.pallas_call(
        kernel,
        out_shape=outs,
        in_specs=in_specs or [vmem] * len(ins),
        out_specs=out_specs or ([vmem] * count if isinstance(outs, (tuple, list)) else vmem),
        scratch_shapes=scratch,
        input_output_aliases=aliases or {},
        compiler_params=pltpu.CompilerParams(vmem_limit_bytes=VMEM_LIMIT),
        cost_estimate=pl.CostEstimate(
            flops=flops, bytes_accessed=size(outs) + size(list(ins)), transcendentals=0),
    )(*ins)


def pair_lists(count):
    even = [pair for low in range(0, count - 1, 2) for pair in ((low, low + 1), (low + 1, low))]
    odd = [pair for low in range(1, count - 1, 2) for pair in ((low, low + 1), (low + 1, low))]
    return [even, odd] if odd else [even]


def exchange(axis, sends):
    lists = pair_lists(lax.axis_size(axis))
    return [lax.ppermute(send, axis, pairs) for send, pairs in zip(sends, lists)]


def diagonal_exchange(sends):
    count_x, count_y = lax.axis_size("gx"), lax.axis_size("gy")
    received = []
    for send, pairs in zip(sends, pair_lists(count_y)):
        flat = []
        for low, high in pairs:
            if low < high:
                for x in range(1, count_x):
                    ends = (x * count_y + low, (x - 1) * count_y + high)
                    flat += [ends, ends[::-1]]
        received.append(lax.ppermute(send, ("gx", "gy"), flat))
    return received


def shift(value, axis, steps):
    count = lax.axis_size(axis)
    pairs = [(i, i + steps) for i in range(count) if 0 <= i + steps < count]
    return lax.ppermute(value, axis, pairs)


def per_device(signal, response, basis, mask, coefficients, extrapolated, dual_grad, dual_sign):
    count, layers, rows, lanes = signal.shape
    assert layers == 1
    s = Shape(basis.shape[0], count, rows, lanes)
    flat = lambda a: a.reshape(count * rows, lanes)
    f32 = lambda *shape: jax.ShapeDtypeStruct(shape, F32)
    bf16 = lambda *shape: jax.ShapeDtypeStruct(shape, BF16)
    vmem = pl.BlockSpec(memory_space=pltpu.VMEM)
    hbm = pl.BlockSpec(memory_space=pltpu.HBM)
    dirs, padded, width = s.padded_dirs, s.padded, s.width
    back = [pltpu.VMEM((dirs, width), F32)]
    dual = f32(3 * s.part_rows, lanes)
    signs = f32(s.part_rows, lanes)
    plane = f32(padded, width)

    after_x = shift(extrapolated, "gx", -1)
    pairs_y = len(pair_lists(lax.axis_size("gy")))
    after_y = exchange("gy", [extrapolated[:, 0, 0]] * pairs_y)
    in_hbm = lambda a: pltpu.with_memory_space_constraint(a, pltpu.HBM)
    line = f32(padded, lanes)
    duals, sign, own, cat, adjoint, column = call(
        functools.partial(load_kernel, s),
        (dual, signs, f32(count * rows, lanes), bf16(dirs, s.depth), bf16(2 * padded, dirs), line),
        [in_hbm(a) for a in
         (flat(extrapolated), basis.T, response[None], dual_grad, dual_sign)],
        [pltpu.VMEM((count, s.directions), F32), pltpu.VMEM((1, count), F32),
         pltpu.VMEM((LANES, round_up(dirs, LANES)), F32), pltpu.VMEM((s.depth, width), BF16),
         pltpu.VMEM((dirs, width), F32), pltpu.SemaphoreType.DMA((4 * rows + 3,))],
        2_000_000_000, in_specs=[hbm] * 5)
    duals, base, inverse, coef, target, from_x, from_y, *sends = call(
        functools.partial(first_kernel, s),
        (dual,) + (plane,) * 5 + (line,) + (plane,) * 2 + (line,) * (2 * pairs_y),
        [duals, sign, cat, adjoint, own, flat(after_x), flat(coefficients), flat(signal),
         mask[0], column] + after_y,
        [pltpu.VMEM((s.depth, width + LANES), BF16), pltpu.VMEM((dirs, width + LANES), F32)] + back,
        2_000_000_000)
    received = exchange("gx", sends[:2])
    received += exchange("gy", sends[2 : 2 + pairs_y])
    received += diagonal_exchange(sends[2 + pairs_y :])
    duals, sign, base, coef, from_x, from_y = call(
        functools.partial(second_kernel, s),
        (dual, signs, plane, plane, plane, line),
        [duals, sign, cat, adjoint, base, inverse, coef, target, from_x, from_y, column] + received,
        [pltpu.VMEM((s.depth, 4 * width), BF16), pltpu.VMEM((dirs, 4 * width), F32)] + back,
        2_000_000_000)
    below_x = shift(from_x, "gx", 1)
    below_y = exchange("gy", [from_y] * pairs_y)
    grad_out, sign_out = call(
        functools.partial(store_kernel, s),
        (f32(*dual_grad.shape), f32(*dual_sign.shape)), (duals, sign),
        [pltpu.SemaphoreType.DMA((4 * rows,))], 2_000_000_000, out_specs=[hbm, hbm])
    coef_out, extra_out = call(
        functools.partial(last_kernel, s),
        (f32(count * rows, lanes), f32(count * rows, lanes)),
        [base, inverse, coef, below_x] + below_y, [], 1_000_000)
    return (coef_out.reshape(signal.shape), extra_out.reshape(signal.shape), grad_out, sign_out)


def solution(mesh):
    cube = P(None, "gx", "gy", None)
    in_specs = (cube, P(), P(), P("gx", "gy", None), cube, cube, P(None, None, "gx", "gy", None), cube)
    out_specs = (cube, cube, P(None, None, "gx", "gy", None), cube)
    return jax.shard_map(per_device, mesh=mesh, in_specs=in_specs, out_specs=out_specs, check_vma=False)
```

```python
import functools

import jax
import jax.numpy as jnp
from jax import lax
from jax.experimental import pallas as pl
from jax.experimental.pallas import tpu as pltpu
from jax.sharding import PartitionSpec as P


STEP_PRIMAL = 0.25
STEP_DUAL = 0.02
TV_WEIGHT = 0.5

F32 = jnp.float32
BF16 = jnp.bfloat16
VMEM_LIMIT = 24 * 1024 * 1024
GROUP = 16
LANES = 128


def round_up(value, unit):
    return -(-value // unit) * unit


def split_two(value):
    high = value.astype(BF16)
    low = (value - high.astype(F32)).astype(BF16)
    return high, low


def put_cat(cat_ref, value, low_row):
    rows, width = value.shape
    high, low = split_two(value)
    cat_ref[0:rows, 0:width] = high
    cat_ref[rows : 2 * rows, 0:width] = high
    cat_ref[low_row : low_row + rows, 0:width] = low


def planes_of(ref, count, rows, padded):
    parts = []
    for row in range(rows):
        part = ref[pl.ds(row, count, stride=rows), :]
        parts.append(jnp.concatenate([part, jnp.zeros((padded - count, part.shape[1]), F32)], 0))
    return jnp.concatenate(parts, 1)


def matmul(left, right):
    return jnp.dot(left, right, preferred_element_type=F32)


def wide_matmul(left_ref, right_ref, out_ref, width):
    for start in range(0, width, 256):
        size = min(256, width - start)
        out_ref[:, start : start + size] = matmul(left_ref[...], right_ref[:, start : start + size])


def harmonics(adjoint_ref, value, padded):
    high, low = split_two(value)
    first = matmul(adjoint_ref[...], high)
    second = matmul(adjoint_ref[0:padded, :], low)
    return first[0:padded] + first[padded : 2 * padded] + second


def last_flags():
    last_x = lax.axis_index("gx") == lax.axis_size("gx") - 1
    last_y = lax.axis_index("gy") == lax.axis_size("gy") - 1
    keep_x = jnp.where(last_x, 0.0, 1.0).astype(F32)
    keep_y = jnp.where(last_y, 0.0, 1.0).astype(F32)
    return keep_x, keep_y


def lane_edge():
    lane = lax.broadcasted_iota(jnp.int32, (GROUP, LANES), 1)
    return jnp.where(lane == LANES - 1, 0.0, 1.0).astype(F32)


def shrunk(step_x, step_y, step_z):
    square = step_x * step_x + step_y * step_y + step_z * step_z
    factor = TV_WEIGHT * lax.rsqrt(jnp.maximum(square, TV_WEIGHT * TV_WEIGHT))
    return step_x * factor, step_y * factor, step_z * factor


def next_lane(value):
    return pltpu.roll(value, LANES - 1, 1)


def previous_lane(value):
    return pltpu.roll(value, 1, 1)


class Shape:
    def __init__(self, directions, count, rows, lanes):
        assert lanes == LANES
        self.directions, self.count, self.rows = directions, count, rows
        self.padded_dirs = round_up(directions, GROUP)
        self.padded = round_up(count + 1, GROUP)
        self.width = rows * lanes
        self.low_row = round_up(2 * self.padded, LANES)
        self.depth = self.low_row + self.padded
        self.groups = self.padded_dirs // GROUP
        self.part_rows = (rows + 1) * self.padded_dirs + 8

    def start(self, part, row):
        return part * self.part_rows + (row + 1) * self.padded_dirs

    def at(self, part, row, index):
        if isinstance(row, int):
            return slice(self.start(part, row) + index * GROUP, self.start(part, row) + (index + 1) * GROUP)
        return pl.ds(pl.multiple_of(self.start(part, row) + index * GROUP, 8), GROUP)

    def lanes(self, row):
        return pl.ds(pl.multiple_of(row * LANES, LANES), LANES)


def load_kernel(s, e_ref, basis_ref, response_ref, grad_ref, sign_ref,
                dual_ref, sign_out, own_ref, cat_ref, adjoint_ref, column_ref,
                basis_in, response_in, padded_ref, e_cat, amp, sems):
    first = [
        pltpu.make_async_copy(basis_ref, basis_in, sems.at[4 * s.rows]),
        pltpu.make_async_copy(response_ref, response_in, sems.at[4 * s.rows + 1]),
        pltpu.make_async_copy(e_ref, own_ref, sems.at[4 * s.rows + 2]),
    ]
    for copy in first:
        copy.start()
    pad_rows = s.padded_dirs - s.directions
    for part in range(4):
        for row in range(s.rows):
            if pad_rows:
                end = s.start(part % 3, row) + s.padded_dirs
                place = sign_out if part == 3 else dual_ref
                place[end - pad_rows : end, :] = jnp.zeros((pad_rows, LANES), F32)

    def copy_of(part, row):
        source = sign_ref.at[:, 0, row] if part == 3 else grad_ref.at[part, :, 0, row]
        place = sign_out if part == 3 else dual_ref
        target = place.at[pl.ds(s.start(part % 3, row), s.directions)]
        return pltpu.make_async_copy(source, target, sems.at[part * s.rows + row])

    for row in range(s.rows):
        for part in (1, 2, 3):
            copy_of(part, row).start()
    for row in range(s.rows):
        copy_of(0, row).start()

    padded_ref[...] = jnp.zeros_like(padded_ref)
    for copy in first:
        copy.wait()
    padded_ref[0 : s.count, 0 : s.directions] = basis_in[...]
    whole = padded_ref[...]
    high, low = split_two(whole)
    adjoint_ref[0 : s.padded, :] = high[0 : s.padded, 0 : s.padded_dirs]
    adjoint_ref[s.padded : 2 * s.padded, :] = low[0 : s.padded, 0 : s.padded_dirs]
    high = high.astype(F32).T[0 : s.padded_dirs]
    low = low.astype(F32).T[0 : s.padded_dirs]
    cat_ref[:, 0:LANES] = (high + pltpu.roll(low, s.padded, 1)).astype(BF16)
    cat_ref[:, s.low_row : s.low_row + s.padded] = high[:, 0 : s.padded].astype(BF16)
    row_index = lax.broadcasted_iota(jnp.int32, (s.padded, LANES), 0)
    lane_index = lax.broadcasted_iota(jnp.int32, (s.padded, LANES), 1)
    spread = jnp.concatenate([response_in[...], jnp.zeros((1, LANES - s.count), F32)], 1)
    picked = jnp.where(row_index == lane_index, spread, 0.0)
    column_ref[...] = jnp.broadcast_to(jnp.sum(picked, 1, keepdims=True), (s.padded, LANES))

    e_cat[...] = jnp.zeros_like(e_cat)
    put_cat(e_cat, planes_of(own_ref, s.count, s.rows, s.padded) * STEP_DUAL, s.low_row)
    wide_matmul(cat_ref, e_cat, amp, s.width)
    edge = lane_edge()

    def update_row(row):
        for part in (1, 2, 3):
            copy_of(part, row).wait()
        for index in range(s.groups):
            here = slice(index * GROUP, (index + 1) * GROUP)
            value = amp[here, s.lanes(row)]
            if not isinstance(row, int):
                dual_ref[s.at(1, row, index), :] += amp[here, s.lanes(row + 1)] - value
            dual_ref[s.at(2, row, index), :] += (next_lane(value) - value) * edge
            sign = sign_out[s.at(0, row, index), :] + value
            sign_out[s.at(0, row, index), :] = jnp.minimum(0.0, sign)

    def step(row, carry):
        update_row(row)
        return carry

    lax.fori_loop(0, s.rows - 1, step, 0)
    update_row(s.rows - 1)
    for row in range(s.rows):
        copy_of(0, row).wait()


def dual_and_adjoints(s, dual_in, sign_in, dual_out, sign_out, cat_ref, e_cat, change, back_ref,
                      adjoint_ref, keep_x, keep_y):
    full = sign_out is not None
    signs = sign_out if full else sign_in
    edge = lane_edge()
    last_row = s.rows - 1
    pairs = [range(row, min(row + 2, s.rows)) for row in range(0, s.rows, 2)]

    def lanes_of(part, row, count=1):
        return slice(part * s.width + row * LANES, part * s.width + (row + count) * LANES)

    def differences(rows):
        parts = [lanes_of(part, rows[0], len(rows)) for part in (range(4) if full else range(1))]
        if not full and last_row in rows:
            parts.append(lanes_of(1, 0))
        for at in parts:
            change[:, at] = matmul(cat_ref[...], e_cat[:, at])

    def shrink_row(row):
        for index in range(s.groups):
            here = slice(index * GROUP, (index + 1) * GROUP)
            step_x = dual_in[s.at(0, row, index), :] + change[here, lanes_of(0, row)]
            step_y, step_z = dual_in[s.at(1, row, index), :], dual_in[s.at(2, row, index), :]
            if full:
                step_y = step_y + change[here, lanes_of(1, row)]
                step_z = step_z + change[here, lanes_of(2, row)]
                sign_out[s.at(0, row, index), :] = jnp.minimum(
                    0.0, sign_in[s.at(0, row, index), :] + change[here, lanes_of(3, row)])
            elif row == last_row:
                step_y = step_y + change[here, lanes_of(1, 0)]
            new_x, new_y, new_z = shrunk(step_x, step_y, step_z)
            dual_out[s.at(0, row, index), :] = new_x
            dual_out[s.at(1, row, index), :] = new_y
            dual_out[s.at(2, row, index), :] = new_z

    def back_row(row):
        for index in range(s.groups):
            here = slice(index * GROUP, (index + 1) * GROUP)
            inner_z = dual_out[s.at(2, row, index), :] * edge
            back = signs[s.at(0, row, index), :] - (inner_z - previous_lane(inner_z))
            back = back - dual_out[s.at(1, row, index), :]
            if row:
                back = back + dual_out[s.at(1, row - 1, index), :]
            back_ref[here, lanes_of(0, row)] = back

    def plane(part, row):
        return dual_out[s.start(part, row) : s.start(part, row) + s.padded_dirs, :]

    from_back, from_x = [], []
    differences(pairs[0])
    for number, rows in enumerate(pairs):
        if number + 1 < len(pairs):
            differences(pairs[number + 1])
        for row in rows:
            shrink_row(row)
        for row in rows:
            back_row(row)
        from_x.append(harmonics(
            adjoint_ref, jnp.concatenate([plane(0, row) for row in rows], 1), s.padded))
        from_back.append(harmonics(
            adjoint_ref, back_ref[:, lanes_of(0, rows[0], len(rows))], s.padded))
    from_back, from_x = jnp.concatenate(from_back, 1), jnp.concatenate(from_x, 1)
    from_y = harmonics(adjoint_ref, plane(1, last_row), s.padded)
    last = from_back[:, s.width - LANES :] + (1.0 - keep_y) * from_y
    total = jnp.concatenate([from_back[:, : s.width - LANES], last], 1) - keep_x * from_x
    return total, from_x, from_y


def weights(s, mask_ref, response_ref):
    mask = jnp.concatenate(
        [mask_ref[row : row + 1, :].astype(F32) for row in range(s.rows)], 1)
    return mask, jnp.concatenate([response_ref[...]] * s.rows, 1)


def is_odd(axis):
    return lax.rem(lax.axis_index(axis), 2) == 1


def to_partners(axis, upward, downward):
    odd = jnp.broadcast_to(is_odd(axis), upward.shape)
    return jnp.where(odd, downward, upward), jnp.where(odd, upward, downward)


def from_partners(axis, over_even, over_odd):
    if over_odd is None:
        over_odd = jnp.zeros_like(over_even)
    odd = jnp.broadcast_to(is_odd(axis), over_even.shape)
    return jnp.where(odd, over_even, over_odd), jnp.where(odd, over_odd, over_even)


def received_at(axis, refs):
    return from_partners(axis, refs[0][...], refs[1][...] if len(refs) > 1 else None)


def first_kernel(s, dual_in, sign_in, cat_ref, adjoint_ref, e_ref, ex_ref, coef_ref, signal_ref,
                 mask_ref, response_ref, *refs):
    pairs_y = len(pair_lists(lax.axis_size("gy")))
    received, refs = refs[:pairs_y], refs[pairs_y:]
    dual_ref, base_ref, inverse_ref, coef_out, target_ref, x_ref, y_ref, *send_refs = refs[:-3]
    e_cat, diff, back_ref = refs[-3:]
    keep_x, keep_y = last_flags()
    here = planes_of(e_ref, s.count, s.rows, s.padded)
    there = planes_of(ex_ref, s.count, s.rows, s.padded)
    _, edge_row = received_at("gy", received)
    edge_row = jnp.concatenate([edge_row, jnp.zeros((s.padded - s.count, LANES), F32)], 0)
    e_cat[2 * s.padded : s.low_row, :] = jnp.zeros((s.low_row - 2 * s.padded, s.width + LANES), BF16)
    put_cat(e_cat, jnp.concatenate(
        [(there - here) * (STEP_DUAL * keep_x),
         (edge_row - here[:, s.width - LANES :]) * (STEP_DUAL * keep_y)], 1), s.low_row)
    total, from_x, from_y = dual_and_adjoints(
        s, dual_in, sign_in, dual_ref, None, cat_ref, e_cat, diff, back_ref, adjoint_ref,
        keep_x, keep_y)
    mask, response = weights(s, mask_ref, response_ref)
    weight = mask * response
    coef = planes_of(coef_ref, s.count, s.rows, s.padded)
    signal = planes_of(signal_ref, s.count, s.rows, s.padded)
    target = STEP_PRIMAL * weight * signal
    inverse = 1.0 / (1.0 + STEP_PRIMAL * weight * response)
    base = coef + target - STEP_PRIMAL * total
    row_index = lax.broadcasted_iota(jnp.int32, (s.padded, s.width), 0)
    ahead = jnp.where(row_index == s.count, mask, 2.0 * base * inverse - coef)
    base_ref[...] = base
    inverse_ref[...] = inverse
    coef_out[...] = coef
    target_ref[...] = target
    x_ref[...] = from_x
    y_ref[...] = from_y
    messages = (
        to_partners("gx", from_x, ahead) + to_partners("gy", from_y, ahead[:, 0:LANES])[:pairs_y]
        + to_partners("gy", from_y, from_x[:, 0:LANES])[:pairs_y])
    for send_ref, message in zip(send_refs, messages):
        send_ref[...] = message


def add_first_row(planes, row):
    return jnp.concatenate([planes[:, 0:LANES] + row, planes[:, LANES:]], 1)


def ahead_of(s, message, own, response):
    row_index = lax.broadcasted_iota(jnp.int32, message.shape, 0)
    mask = message[s.count : s.count + 1, :]
    inverse = 1.0 / (1.0 + STEP_PRIMAL * (mask * response) * response)
    return jnp.where(row_index < s.count, message - (2.0 * STEP_PRIMAL) * inverse * own, 0.0)


def second_kernel(s, dual_in, sign_in, cat_ref, adjoint_ref, base_ref, inverse_ref, coef_ref, target_ref,
                  x_ref, y_ref, response_ref, *refs):
    *received, dual_ref, sign_ref, base_out, coef_out, x_out, y_out = refs[:-3]
    e_cat, change, back_ref = refs[-3:]
    pairs_y = (len(received) - 2) // 2
    keep_x, keep_y = last_flags()
    below, above = received_at("gx", received[:2])
    below_y, above_y = received_at("gy", received[2 : 2 + pairs_y])
    below_d, above_d = received_at("gy", received[2 + pairs_y :])
    response = response_ref[...]
    coef = coef_ref[...]
    updated = (base_ref[...] - STEP_PRIMAL * add_first_row(below, below_y)) * inverse_ref[...]
    here = 2.0 * updated - coef
    wide = jnp.concatenate([response] * s.rows, 1)
    there = ahead_of(s, above, add_first_row(x_ref[...], below_d), wide)
    edge_row = ahead_of(s, above_y, y_ref[...] + above_d, response)
    e_cat[2 * s.padded : s.low_row, :] = jnp.zeros((s.low_row - 2 * s.padded, 4 * s.width), BF16)
    edge = lane_edge()[0:1]
    planes = [here[:, row * LANES : (row + 1) * LANES] for row in range(s.rows)]
    along_y = jnp.concatenate([here[:, LANES:], edge_row], 1) - here
    along_y = jnp.concatenate(
        [along_y[:, : s.width - LANES], keep_y * along_y[:, s.width - LANES :]], 1)
    along_z = jnp.concatenate([(next_lane(plane) - plane) * edge for plane in planes], 1)
    put_cat(e_cat, STEP_DUAL * jnp.concatenate(
        [(there - here) * keep_x, along_y, along_z, here], 1), s.low_row)
    total, from_x, from_y = dual_and_adjoints(
        s, dual_in, sign_in, dual_ref, sign_ref, cat_ref, e_cat, change, back_ref, adjoint_ref,
        keep_x, keep_y)
    base_out[...] = updated + target_ref[...] - STEP_PRIMAL * total
    coef_out[...] = updated
    x_out[...] = from_x
    y_out[...] = from_y


def store_kernel(s, dual_ref, sign_in, grad_ref, sign_ref, sems):
    copies = []
    for row in range(s.rows):
        for part in range(3):
            copies.append(pltpu.make_async_copy(
                dual_ref.at[pl.ds(s.start(part, row), s.directions)], grad_ref.at[part, :, 0, row],
                sems.at[part * s.rows + row]))
        copies.append(pltpu.make_async_copy(
            sign_in.at[pl.ds(s.start(0, row), s.directions)], sign_ref.at[:, 0, row],
            sems.at[3 * s.rows + row]))
    for copy in copies:
        copy.start()
    for copy in copies:
        copy.wait()


def last_kernel(s, base_ref, inverse_ref, coef_ref, x_ref, *refs):
    *received, coef_out, extra_out = refs
    below_y, _ = received_at("gy", received)
    total = add_first_row(x_ref[...], below_y)
    updated = (base_ref[...] - STEP_PRIMAL * total) * inverse_ref[...]
    extra = 2.0 * updated - coef_ref[...]
    for row in range(s.rows):
        at = slice(row * LANES, (row + 1) * LANES)
        coef_out[pl.ds(row, s.count, stride=s.rows), :] = updated[0 : s.count, at]
        extra_out[pl.ds(row, s.count, stride=s.rows), :] = extra[0 : s.count, at]


def call(kernel, outs, ins, scratch, flops, in_specs=None, out_specs=None, aliases=None):
    vmem = pl.BlockSpec(memory_space=pltpu.VMEM)
    count = len(outs) if isinstance(outs, (tuple, list)) else 1
    size = lambda arrays: sum(a.size * a.dtype.itemsize for a in jax.tree.leaves(arrays))
    return pl.pallas_call(
        kernel,
        out_shape=outs,
        in_specs=in_specs or [vmem] * len(ins),
        out_specs=out_specs or ([vmem] * count if isinstance(outs, (tuple, list)) else vmem),
        scratch_shapes=scratch,
        input_output_aliases=aliases or {},
        compiler_params=pltpu.CompilerParams(vmem_limit_bytes=VMEM_LIMIT),
        cost_estimate=pl.CostEstimate(
            flops=flops, bytes_accessed=size(outs) + size(list(ins)), transcendentals=0),
    )(*ins)


def pair_lists(count):
    even = [pair for low in range(0, count - 1, 2) for pair in ((low, low + 1), (low + 1, low))]
    odd = [pair for low in range(1, count - 1, 2) for pair in ((low, low + 1), (low + 1, low))]
    return [even, odd] if odd else [even]


def exchange(axis, sends):
    lists = pair_lists(lax.axis_size(axis))
    return [lax.ppermute(send, axis, pairs) for send, pairs in zip(sends, lists)]


def diagonal_exchange(sends):
    count_x, count_y = lax.axis_size("gx"), lax.axis_size("gy")
    received = []
    for send, pairs in zip(sends, pair_lists(count_y)):
        flat = []
        for low, high in pairs:
            if low < high:
                for x in range(1, count_x):
                    ends = (x * count_y + low, (x - 1) * count_y + high)
                    flat += [ends, ends[::-1]]
        received.append(lax.ppermute(send, ("gx", "gy"), flat))
    return received


def shift(value, axis, steps):
    count = lax.axis_size(axis)
    pairs = [(i, i + steps) for i in range(count) if 0 <= i + steps < count]
    return lax.ppermute(value, axis, pairs)


def per_device(signal, response, basis, mask, coefficients, extrapolated, dual_grad, dual_sign):
    count, layers, rows, lanes = signal.shape
    assert layers == 1
    s = Shape(basis.shape[0], count, rows, lanes)
    flat = lambda a: a.reshape(count * rows, lanes)
    f32 = lambda *shape: jax.ShapeDtypeStruct(shape, F32)
    bf16 = lambda *shape: jax.ShapeDtypeStruct(shape, BF16)
    vmem = pl.BlockSpec(memory_space=pltpu.VMEM)
    hbm = pl.BlockSpec(memory_space=pltpu.HBM)
    dirs, padded, width = s.padded_dirs, s.padded, s.width
    back = [pltpu.VMEM((dirs, width), F32)]
    dual = f32(3 * s.part_rows, lanes)
    signs = f32(s.part_rows, lanes)
    plane = f32(padded, width)

    after_x = shift(extrapolated, "gx", -1)
    pairs_y = len(pair_lists(lax.axis_size("gy")))
    after_y = exchange("gy", [extrapolated[:, 0, 0]] * pairs_y)
    in_hbm = lambda a: pltpu.with_memory_space_constraint(a, pltpu.HBM)
    line = f32(padded, lanes)
    duals, sign, own, cat, adjoint, column = call(
        functools.partial(load_kernel, s),
        (dual, signs, f32(count * rows, lanes), bf16(dirs, s.depth), bf16(2 * padded, dirs), line),
        [in_hbm(a) for a in
         (flat(extrapolated), basis.T, response[None], dual_grad, dual_sign)],
        [pltpu.VMEM((count, s.directions), F32), pltpu.VMEM((1, count), F32),
         pltpu.VMEM((LANES, round_up(dirs, LANES)), F32), pltpu.VMEM((s.depth, width), BF16),
         pltpu.VMEM((dirs, width), F32), pltpu.SemaphoreType.DMA((4 * rows + 3,))],
        2_000_000_000, in_specs=[hbm] * 5)
    duals, base, inverse, coef, target, from_x, from_y, *sends = call(
        functools.partial(first_kernel, s),
        (dual,) + (plane,) * 5 + (line,) + (plane,) * 2 + (line,) * (2 * pairs_y),
        [duals, sign, cat, adjoint, own, flat(after_x), flat(coefficients), flat(signal),
         mask[0], column] + after_y,
        [pltpu.VMEM((s.depth, width + LANES), BF16), pltpu.VMEM((dirs, width + LANES), F32)] + back,
        2_000_000_000)
    received = exchange("gx", sends[:2])
    received += exchange("gy", sends[2 : 2 + pairs_y])
    received += diagonal_exchange(sends[2 + pairs_y :])
    duals, sign, base, coef, from_x, from_y = call(
        functools.partial(second_kernel, s),
        (dual, signs, plane, plane, plane, line),
        [duals, sign, cat, adjoint, base, inverse, coef, target, from_x, from_y, column] + received,
        [pltpu.VMEM((s.depth, 4 * width), BF16), pltpu.VMEM((dirs, 4 * width), F32)] + back,
        2_000_000_000)
    below_x = shift(from_x, "gx", 1)
    below_y = exchange("gy", [from_y] * pairs_y)
    grad_out, sign_out = call(
        functools.partial(store_kernel, s),
        (f32(*dual_grad.shape), f32(*dual_sign.shape)), (duals, sign),
        [pltpu.SemaphoreType.DMA((4 * rows,))], 2_000_000_000, out_specs=[hbm, hbm])
    coef_out, extra_out = call(
        functools.partial(last_kernel, s),
        (f32(count * rows, lanes), f32(count * rows, lanes)),
        [base, inverse, coef, below_x] + below_y, [], 1_000_000)
    return (coef_out.reshape(signal.shape), extra_out.reshape(signal.shape), grad_out, sign_out)


def solution(mesh):
    cube = P(None, "gx", "gy", None)
    in_specs = (cube, P(), P(), P("gx", "gy", None), cube, cube, P(None, None, "gx", "gy", None), cube)
    out_specs = (cube, cube, P(None, None, "gx", "gy", None), cube)
    return jax.shard_map(per_device, mesh=mesh, in_specs=in_specs, out_specs=out_specs, check_vma=False)
```

```python
import functools

import jax
import jax.numpy as jnp
from jax import lax
from jax.experimental import pallas as pl
from jax.experimental.pallas import tpu as pltpu
from jax.sharding import PartitionSpec as P


STEP_PRIMAL = 0.25
STEP_DUAL = 0.02
TV_WEIGHT = 0.5

F32 = jnp.float32
BF16 = jnp.bfloat16
VMEM_LIMIT = 24 * 1024 * 1024
GROUP = 16
LANES = 128


def round_up(value, unit):
    return -(-value // unit) * unit


def split_two(value):
    high = value.astype(BF16)
    low = (value - high.astype(F32)).astype(BF16)
    return high, low


def put_cat(cat_ref, value, low_row):
    rows, width = value.shape
    high, low = split_two(value)
    cat_ref[0:rows, 0:width] = high
    cat_ref[rows : 2 * rows, 0:width] = high
    cat_ref[low_row : low_row + rows, 0:width] = low


def planes_of(ref, count, rows, padded):
    parts = []
    for row in range(rows):
        part = ref[pl.ds(row, count, stride=rows), :]
        parts.append(jnp.concatenate([part, jnp.zeros((padded - count, part.shape[1]), F32)], 0))
    return jnp.concatenate(parts, 1)


def matmul(left, right):
    return jnp.dot(left, right, preferred_element_type=F32)


def wide_matmul(left_ref, right_ref, out_ref, width):
    for start in range(0, width, 256):
        size = min(256, width - start)
        out_ref[:, start : start + size] = matmul(left_ref[...], right_ref[:, start : start + size])


def harmonics(adjoint_ref, value, padded):
    high, low = split_two(value)
    first = matmul(adjoint_ref[...], high)
    second = matmul(adjoint_ref[0:padded, :], low)
    return first[0:padded] + first[padded : 2 * padded] + second


def last_flags():
    last_x = lax.axis_index("gx") == lax.axis_size("gx") - 1
    last_y = lax.axis_index("gy") == lax.axis_size("gy") - 1
    keep_x = jnp.where(last_x, 0.0, 1.0).astype(F32)
    keep_y = jnp.where(last_y, 0.0, 1.0).astype(F32)
    return keep_x, keep_y


def lane_edge():
    lane = lax.broadcasted_iota(jnp.int32, (GROUP, LANES), 1)
    return jnp.where(lane == LANES - 1, 0.0, 1.0).astype(F32)


def shrunk(step_x, step_y, step_z):
    square = step_x * step_x + step_y * step_y + step_z * step_z
    factor = TV_WEIGHT * lax.rsqrt(jnp.maximum(square, TV_WEIGHT * TV_WEIGHT))
    return step_x * factor, step_y * factor, step_z * factor


def next_lane(value):
    return pltpu.roll(value, LANES - 1, 1)


def previous_lane(value):
    return pltpu.roll(value, 1, 1)


class Shape:
    def __init__(self, directions, count, rows, lanes):
        assert lanes == LANES
        self.directions, self.count, self.rows = directions, count, rows
        self.padded_dirs = round_up(directions, GROUP)
        self.padded = round_up(count + 1, GROUP)
        self.width = rows * lanes
        self.low_row = round_up(2 * self.padded, LANES)
        self.depth = self.low_row + self.padded
        self.groups = self.padded_dirs // GROUP
        self.part_rows = (rows + 1) * self.padded_dirs + 8

    def start(self, part, row):
        return part * self.part_rows + (row + 1) * self.padded_dirs

    def at(self, part, row, index):
        if isinstance(row, int):
            return slice(self.start(part, row) + index * GROUP, self.start(part, row) + (index + 1) * GROUP)
        return pl.ds(pl.multiple_of(self.start(part, row) + index * GROUP, 8), GROUP)

    def lanes(self, row):
        return pl.ds(pl.multiple_of(row * LANES, LANES), LANES)


def load_kernel(s, e_ref, basis_ref, response_ref, grad_ref, sign_ref,
                dual_ref, sign_out, own_ref, cat_ref, adjoint_ref, column_ref,
                basis_in, response_in, padded_ref, e_cat, amp, sems):
    first = [
        pltpu.make_async_copy(basis_ref, basis_in, sems.at[4 * s.rows]),
        pltpu.make_async_copy(response_ref, response_in, sems.at[4 * s.rows + 1]),
        pltpu.make_async_copy(e_ref, own_ref, sems.at[4 * s.rows + 2]),
    ]
    for copy in first:
        copy.start()
    pad_rows = s.padded_dirs - s.directions
    for part in range(4):
        for row in range(s.rows):
            if pad_rows:
                end = s.start(part % 3, row) + s.padded_dirs
                place = sign_out if part == 3 else dual_ref
                place[end - pad_rows : end, :] = jnp.zeros((pad_rows, LANES), F32)

    def copy_of(part, row):
        source = sign_ref.at[:, 0, row] if part == 3 else grad_ref.at[part, :, 0, row]
        place = sign_out if part == 3 else dual_ref
        target = place.at[pl.ds(s.start(part % 3, row), s.directions)]
        return pltpu.make_async_copy(source, target, sems.at[part * s.rows + row])

    for row in range(s.rows):
        for part in (1, 2, 3):
            copy_of(part, row).start()
    for row in range(s.rows):
        copy_of(0, row).start()

    padded_ref[...] = jnp.zeros_like(padded_ref)
    for copy in first:
        copy.wait()
    padded_ref[0 : s.count, 0 : s.directions] = basis_in[...]
    whole = padded_ref[...]
    high, low = split_two(whole)
    adjoint_ref[0 : s.padded, :] = high[0 : s.padded, 0 : s.padded_dirs]
    adjoint_ref[s.padded : 2 * s.padded, :] = low[0 : s.padded, 0 : s.padded_dirs]
    high = high.astype(F32).T[0 : s.padded_dirs]
    low = low.astype(F32).T[0 : s.padded_dirs]
    cat_ref[:, 0:LANES] = (high + pltpu.roll(low, s.padded, 1)).astype(BF16)
    cat_ref[:, s.low_row : s.low_row + s.padded] = high[:, 0 : s.padded].astype(BF16)
    row_index = lax.broadcasted_iota(jnp.int32, (s.padded, LANES), 0)
    lane_index = lax.broadcasted_iota(jnp.int32, (s.padded, LANES), 1)
    spread = jnp.concatenate([response_in[...], jnp.zeros((1, LANES - s.count), F32)], 1)
    picked = jnp.where(row_index == lane_index, spread, 0.0)
    column_ref[...] = jnp.broadcast_to(jnp.sum(picked, 1, keepdims=True), (s.padded, LANES))

    e_cat[...] = jnp.zeros_like(e_cat)
    put_cat(e_cat, planes_of(own_ref, s.count, s.rows, s.padded) * STEP_DUAL, s.low_row)
    wide_matmul(cat_ref, e_cat, amp, s.width)
    edge = lane_edge()

    def update_row(row):
        for part in (1, 2, 3):
            copy_of(part, row).wait()
        for index in range(s.groups):
            here = slice(index * GROUP, (index + 1) * GROUP)
            value = amp[here, s.lanes(row)]
            if not isinstance(row, int):
                dual_ref[s.at(1, row, index), :] += amp[here, s.lanes(row + 1)] - value
            dual_ref[s.at(2, row, index), :] += (next_lane(value) - value) * edge
            sign = sign_out[s.at(0, row, index), :] + value
            sign_out[s.at(0, row, index), :] = jnp.minimum(0.0, sign)

    def step(row, carry):
        update_row(row)
        return carry

    lax.fori_loop(0, s.rows - 1, step, 0)
    update_row(s.rows - 1)
    for row in range(s.rows):
        copy_of(0, row).wait()


def row_pairs(s):
    return [range(row, min(row + 2, s.rows)) for row in range(0, s.rows, 2)]


def back_rows(s, rows, signs, dual_ref, back_ref):
    edge = lane_edge()
    for row in rows:
        for index in range(s.groups):
            here = slice(index * GROUP, (index + 1) * GROUP)
            inner_z = dual_ref[s.at(2, row, index), :] * edge
            back = signs[s.at(0, row, index), :] - (inner_z - previous_lane(inner_z))
            back = back - dual_ref[s.at(1, row, index), :]
            if row:
                back = back + dual_ref[s.at(1, row - 1, index), :]
            back_ref[here, row * LANES : (row + 1) * LANES] = back


def back_harmonics(s, rows, adjoint_ref, back_ref):
    at = slice(rows[0] * LANES, (rows[-1] + 1) * LANES)
    return harmonics(adjoint_ref, back_ref[:, at], s.padded)


def whole_adjoint(s, from_back, from_x, from_y, keep_x, keep_y):
    last = from_back[:, s.width - LANES :] + (1.0 - keep_y) * from_y
    return jnp.concatenate([from_back[:, : s.width - LANES], last], 1) - keep_x * from_x


def dual_and_adjoints(s, dual_in, sign_in, dual_out, sign_out, cat_ref, e_cat, change, back_ref,
                      adjoint_ref):
    full = sign_out is not None
    last_row = s.rows - 1
    pairs = row_pairs(s)

    def lanes_of(part, row, count=1):
        return slice(part * s.width + row * LANES, part * s.width + (row + count) * LANES)

    def differences(rows):
        parts = [lanes_of(part, rows[0], len(rows)) for part in (range(4) if full else range(1))]
        if not full and last_row in rows:
            parts.append(lanes_of(1, 0))
        for at in parts:
            change[:, at] = matmul(cat_ref[...], e_cat[:, at])

    def shrink_row(row):
        for index in range(s.groups):
            here = slice(index * GROUP, (index + 1) * GROUP)
            step_x = dual_in[s.at(0, row, index), :] + change[here, lanes_of(0, row)]
            step_y, step_z = dual_in[s.at(1, row, index), :], dual_in[s.at(2, row, index), :]
            if full:
                step_y = step_y + change[here, lanes_of(1, row)]
                step_z = step_z + change[here, lanes_of(2, row)]
                sign_out[s.at(0, row, index), :] = jnp.minimum(
                    0.0, sign_in[s.at(0, row, index), :] + change[here, lanes_of(3, row)])
            elif row == last_row:
                step_y = step_y + change[here, lanes_of(1, 0)]
            new_x, new_y, new_z = shrunk(step_x, step_y, step_z)
            dual_out[s.at(0, row, index), :] = new_x
            dual_out[s.at(1, row, index), :] = new_y
            dual_out[s.at(2, row, index), :] = new_z

    def plane(part, row):
        return dual_out[s.start(part, row) : s.start(part, row) + s.padded_dirs, :]

    from_back, from_x = [], []
    differences(pairs[0])
    for number, rows in enumerate(pairs):
        if number + 1 < len(pairs):
            differences(pairs[number + 1])
        for row in rows:
            shrink_row(row)
        if not full:
            back_rows(s, rows, sign_in, dual_out, back_ref)
        from_x.append(harmonics(
            adjoint_ref, jnp.concatenate([plane(0, row) for row in rows], 1), s.padded))
        if not full:
            from_back.append(back_harmonics(s, rows, adjoint_ref, back_ref))
    from_y = harmonics(adjoint_ref, plane(1, last_row), s.padded)
    from_back = None if full else jnp.concatenate(from_back, 1)
    return from_back, jnp.concatenate(from_x, 1), from_y


def weights(s, mask_ref, response_ref):
    mask = jnp.concatenate(
        [mask_ref[row : row + 1, :].astype(F32) for row in range(s.rows)], 1)
    return mask, jnp.concatenate([response_ref[...]] * s.rows, 1)


def is_odd(axis):
    return lax.rem(lax.axis_index(axis), 2) == 1


def to_partners(axis, upward, downward):
    odd = jnp.broadcast_to(is_odd(axis), upward.shape)
    return jnp.where(odd, downward, upward), jnp.where(odd, upward, downward)


def from_partners(axis, over_even, over_odd):
    if over_odd is None:
        over_odd = jnp.zeros_like(over_even)
    odd = jnp.broadcast_to(is_odd(axis), over_even.shape)
    return jnp.where(odd, over_even, over_odd), jnp.where(odd, over_odd, over_even)


def received_at(axis, refs):
    return from_partners(axis, refs[0][...], refs[1][...] if len(refs) > 1 else None)


def first_kernel(s, dual_in, sign_in, cat_ref, adjoint_ref, e_ref, ex_ref, coef_ref, signal_ref,
                 mask_ref, response_ref, *refs):
    pairs_y = len(pair_lists(lax.axis_size("gy")))
    received, refs = refs[:pairs_y], refs[pairs_y:]
    dual_ref, base_ref, inverse_ref, coef_out, target_ref, x_ref, y_ref, *send_refs = refs[:-3]
    e_cat, diff, back_ref = refs[-3:]
    keep_x, keep_y = last_flags()
    here = planes_of(e_ref, s.count, s.rows, s.padded)
    there = planes_of(ex_ref, s.count, s.rows, s.padded)
    _, edge_row = received_at("gy", received)
    edge_row = jnp.concatenate([edge_row, jnp.zeros((s.padded - s.count, LANES), F32)], 0)
    e_cat[2 * s.padded : s.low_row, :] = jnp.zeros((s.low_row - 2 * s.padded, s.width + LANES), BF16)
    put_cat(e_cat, jnp.concatenate(
        [(there - here) * (STEP_DUAL * keep_x),
         (edge_row - here[:, s.width - LANES :]) * (STEP_DUAL * keep_y)], 1), s.low_row)
    from_back, from_x, from_y = dual_and_adjoints(
        s, dual_in, sign_in, dual_ref, None, cat_ref, e_cat, diff, back_ref, adjoint_ref)
    total = whole_adjoint(s, from_back, from_x, from_y, keep_x, keep_y)
    mask, response = weights(s, mask_ref, response_ref)
    weight = mask * response
    coef = planes_of(coef_ref, s.count, s.rows, s.padded)
    signal = planes_of(signal_ref, s.count, s.rows, s.padded)
    target = STEP_PRIMAL * weight * signal
    inverse = 1.0 / (1.0 + STEP_PRIMAL * weight * response)
    base = coef + target - STEP_PRIMAL * total
    row_index = lax.broadcasted_iota(jnp.int32, (s.padded, s.width), 0)
    ahead = jnp.where(row_index == s.count, mask, 2.0 * base * inverse - coef)
    base_ref[...] = base
    inverse_ref[...] = inverse
    coef_out[...] = coef
    target_ref[...] = target
    x_ref[...] = from_x
    y_ref[...] = from_y
    messages = (
        to_partners("gx", from_x, ahead) + to_partners("gy", from_y, ahead[:, 0:LANES])[:pairs_y]
        + to_partners("gy", from_y, from_x[:, 0:LANES])[:pairs_y])
    for send_ref, message in zip(send_refs, messages):
        send_ref[...] = message


def add_first_row(planes, row):
    return jnp.concatenate([planes[:, 0:LANES] + row, planes[:, LANES:]], 1)


def ahead_of(s, message, own, response):
    row_index = lax.broadcasted_iota(jnp.int32, message.shape, 0)
    mask = message[s.count : s.count + 1, :]
    inverse = 1.0 / (1.0 + STEP_PRIMAL * (mask * response) * response)
    return jnp.where(row_index < s.count, message - (2.0 * STEP_PRIMAL) * inverse * own, 0.0)


def second_kernel(s, dual_in, sign_in, cat_ref, adjoint_ref, base_ref, inverse_ref, coef_ref,
                  x_ref, y_ref, response_ref, *refs):
    *received, dual_ref, sign_ref, coef_out, x_out, y_out, e_cat, change = refs
    pairs_y = (len(received) - 2) // 2
    keep_x, keep_y = last_flags()
    below, above = received_at("gx", received[:2])
    below_y, above_y = received_at("gy", received[2 : 2 + pairs_y])
    below_d, above_d = received_at("gy", received[2 + pairs_y :])
    response = response_ref[...]
    coef = coef_ref[...]
    updated = (base_ref[...] - STEP_PRIMAL * add_first_row(below, below_y)) * inverse_ref[...]
    here = 2.0 * updated - coef
    wide = jnp.concatenate([response] * s.rows, 1)
    there = ahead_of(s, above, add_first_row(x_ref[...], below_d), wide)
    edge_row = ahead_of(s, above_y, y_ref[...] + above_d, response)
    e_cat[2 * s.padded : s.low_row, :] = jnp.zeros((s.low_row - 2 * s.padded, 4 * s.width), BF16)
    edge = lane_edge()[0:1]
    planes = [here[:, row * LANES : (row + 1) * LANES] for row in range(s.rows)]
    along_y = jnp.concatenate([here[:, LANES:], edge_row], 1) - here
    along_y = jnp.concatenate(
        [along_y[:, : s.width - LANES], keep_y * along_y[:, s.width - LANES :]], 1)
    along_z = jnp.concatenate([(next_lane(plane) - plane) * edge for plane in planes], 1)
    put_cat(e_cat, STEP_DUAL * jnp.concatenate(
        [(there - here) * keep_x, along_y, along_z, here], 1), s.low_row)
    _, from_x, from_y = dual_and_adjoints(
        s, dual_in, sign_in, dual_ref, sign_ref, cat_ref, e_cat, change, None, adjoint_ref)
    coef_out[...] = updated
    x_out[...] = from_x
    y_out[...] = from_y


def close_kernel(s, dual_ref, sign_in, adjoint_ref, coef_ref, target_ref, x_ref, y_ref,
                 base_ref, grad_ref, sign_ref, back_ref, sems):
    copies = []
    for row in range(s.rows):
        for part in range(3):
            copies.append(pltpu.make_async_copy(
                dual_ref.at[pl.ds(s.start(part, row), s.directions)], grad_ref.at[part, :, 0, row],
                sems.at[part * s.rows + row]))
        copies.append(pltpu.make_async_copy(
            sign_in.at[pl.ds(s.start(0, row), s.directions)], sign_ref.at[:, 0, row],
            sems.at[3 * s.rows + row]))
    for copy in copies:
        copy.start()
    keep_x, keep_y = last_flags()
    from_back = []
    for rows in row_pairs(s):
        back_rows(s, rows, sign_in, dual_ref, back_ref)
        from_back.append(back_harmonics(s, rows, adjoint_ref, back_ref))
    total = whole_adjoint(
        s, jnp.concatenate(from_back, 1), x_ref[...], y_ref[...], keep_x, keep_y)
    base_ref[...] = coef_ref[...] + target_ref[...] - STEP_PRIMAL * total
    for copy in copies:
        copy.wait()


def last_kernel(s, base_ref, inverse_ref, coef_ref, x_ref, *refs):
    *received, coef_out, extra_out = refs
    below_y, _ = received_at("gy", received)
    total = add_first_row(x_ref[...], below_y)
    updated = (base_ref[...] - STEP_PRIMAL * total) * inverse_ref[...]
    extra = 2.0 * updated - coef_ref[...]
    for row in range(s.rows):
        at = slice(row * LANES, (row + 1) * LANES)
        coef_out[pl.ds(row, s.count, stride=s.rows), :] = updated[0 : s.count, at]
        extra_out[pl.ds(row, s.count, stride=s.rows), :] = extra[0 : s.count, at]


def call(kernel, outs, ins, scratch, flops, in_specs=None, out_specs=None, aliases=None):
    vmem = pl.BlockSpec(memory_space=pltpu.VMEM)
    count = len(outs) if isinstance(outs, (tuple, list)) else 1
    size = lambda arrays: sum(a.size * a.dtype.itemsize for a in jax.tree.leaves(arrays))
    return pl.pallas_call(
        kernel,
        out_shape=outs,
        in_specs=in_specs or [vmem] * len(ins),
        out_specs=out_specs or ([vmem] * count if isinstance(outs, (tuple, list)) else vmem),
        scratch_shapes=scratch,
        input_output_aliases=aliases or {},
        compiler_params=pltpu.CompilerParams(vmem_limit_bytes=VMEM_LIMIT),
        cost_estimate=pl.CostEstimate(
            flops=flops, bytes_accessed=size(outs) + size(list(ins)), transcendentals=0),
    )(*ins)


def pair_lists(count):
    even = [pair for low in range(0, count - 1, 2) for pair in ((low, low + 1), (low + 1, low))]
    odd = [pair for low in range(1, count - 1, 2) for pair in ((low, low + 1), (low + 1, low))]
    return [even, odd] if odd else [even]


def exchange(axis, sends):
    lists = pair_lists(lax.axis_size(axis))
    return [lax.ppermute(send, axis, pairs) for send, pairs in zip(sends, lists)]


def diagonal_exchange(sends):
    count_x, count_y = lax.axis_size("gx"), lax.axis_size("gy")
    received = []
    for send, pairs in zip(sends, pair_lists(count_y)):
        flat = []
        for low, high in pairs:
            if low < high:
                for x in range(1, count_x):
                    ends = (x * count_y + low, (x - 1) * count_y + high)
                    flat += [ends, ends[::-1]]
        received.append(lax.ppermute(send, ("gx", "gy"), flat))
    return received


def shift(value, axis, steps):
    count = lax.axis_size(axis)
    pairs = [(i, i + steps) for i in range(count) if 0 <= i + steps < count]
    return lax.ppermute(value, axis, pairs)


def per_device(signal, response, basis, mask, coefficients, extrapolated, dual_grad, dual_sign):
    count, layers, rows, lanes = signal.shape
    assert layers == 1
    s = Shape(basis.shape[0], count, rows, lanes)
    flat = lambda a: a.reshape(count * rows, lanes)
    f32 = lambda *shape: jax.ShapeDtypeStruct(shape, F32)
    bf16 = lambda *shape: jax.ShapeDtypeStruct(shape, BF16)
    vmem = pl.BlockSpec(memory_space=pltpu.VMEM)
    hbm = pl.BlockSpec(memory_space=pltpu.HBM)
    dirs, padded, width = s.padded_dirs, s.padded, s.width
    back = [pltpu.VMEM((dirs, width), F32)]
    dual = f32(3 * s.part_rows, lanes)
    signs = f32(s.part_rows, lanes)
    plane = f32(padded, width)

    after_x = shift(extrapolated, "gx", -1)
    pairs_y = len(pair_lists(lax.axis_size("gy")))
    after_y = exchange("gy", [extrapolated[:, 0, 0]] * pairs_y)
    in_hbm = lambda a: pltpu.with_memory_space_constraint(a, pltpu.HBM)
    line = f32(padded, lanes)
    duals, sign, own, cat, adjoint, column = call(
        functools.partial(load_kernel, s),
        (dual, signs, f32(count * rows, lanes), bf16(dirs, s.depth), bf16(2 * padded, dirs), line),
        [in_hbm(a) for a in
         (flat(extrapolated), basis.T, response[None], dual_grad, dual_sign)],
        [pltpu.VMEM((count, s.directions), F32), pltpu.VMEM((1, count), F32),
         pltpu.VMEM((LANES, round_up(dirs, LANES)), F32), pltpu.VMEM((s.depth, width), BF16),
         pltpu.VMEM((dirs, width), F32), pltpu.SemaphoreType.DMA((4 * rows + 3,))],
        2_000_000_000, in_specs=[hbm] * 5)
    duals, base, inverse, coef, target, from_x, from_y, *sends = call(
        functools.partial(first_kernel, s),
        (dual,) + (plane,) * 5 + (line,) + (plane,) * 2 + (line,) * (2 * pairs_y),
        [duals, sign, cat, adjoint, own, flat(after_x), flat(coefficients), flat(signal),
         mask[0], column] + after_y,
        [pltpu.VMEM((s.depth, width + LANES), BF16), pltpu.VMEM((dirs, width + LANES), F32)] + back,
        2_000_000_000)
    received = exchange("gx", sends[:2])
    received += exchange("gy", sends[2 : 2 + pairs_y])
    received += diagonal_exchange(sends[2 + pairs_y :])
    duals, sign, coef, from_x, from_y = call(
        functools.partial(second_kernel, s),
        (dual, signs, plane, plane, line),
        [duals, sign, cat, adjoint, base, inverse, coef, from_x, from_y, column] + received,
        [pltpu.VMEM((s.depth, 4 * width), BF16), pltpu.VMEM((dirs, 4 * width), F32)],
        2_000_000_000)
    below_x = shift(from_x, "gx", 1)
    below_y = exchange("gy", [from_y] * pairs_y)
    base, grad_out, sign_out = call(
        functools.partial(close_kernel, s),
        (plane, f32(*dual_grad.shape), f32(*dual_sign.shape)),
        [duals, sign, adjoint, coef, target, from_x, from_y],
        back + [pltpu.SemaphoreType.DMA((4 * rows,))], 2_000_000_000,
        out_specs=[vmem, hbm, hbm])
    coef_out, extra_out = call(
        functools.partial(last_kernel, s),
        (f32(count * rows, lanes), f32(count * rows, lanes)),
        [base, inverse, coef, below_x] + below_y, [], 1_000_000)
    return (coef_out.reshape(signal.shape), extra_out.reshape(signal.shape), grad_out, sign_out)


def solution(mesh):
    cube = P(None, "gx", "gy", None)
    in_specs = (cube, P(), P(), P("gx", "gy", None), cube, cube, P(None, None, "gx", "gy", None), cube)
    out_specs = (cube, cube, P(None, None, "gx", "gy", None), cube)
    return jax.shard_map(per_device, mesh=mesh, in_specs=in_specs, out_specs=out_specs, check_vma=False)
```
